8 devices in a mesh: dp: 2 (over z, y), tp: 4 (over x, core).
Axes of the slice: x: 2, y: 2, z: 1, core: 2. Of those that a mesh axis runs over, the one named last changes fastest.
Arguments:
- hidden: bfloat16 [4, 512, 7168], P('dp', 'tp'), parts along dimension 0
- lengths: int32 [4], P('dp'), parts along dimension 0
- rope_cos: float32 [4, 512, 32], P('dp'), parts along dimension 0
- rope_sin: float32 [4, 512, 32], P('dp'), parts along dimension 0
- cache_lat: bfloat16 [4, 1024, 512], P('dp'), parts along dimension 0
- cache_pe: bfloat16 [4, 1024, 64], P('dp'), parts along dimension 0
- norm_in: float32 [7168], replicated
- w_dq: bfloat16 [7168, 1536], replicated
- norm_q: float32 [1536], replicated
- w_dkv: bfloat16 [7168, 576], replicated
- norm_kv: float32 [512], replicated
- w_uq: bfloat16 [1536, 128, 192], P(None, 'tp')
- w_uk: bfloat16 [512, 128, 128], P(None, 'tp')
- w_uv: bfloat16 [512, 128, 128], P(None, 'tp')
- w_out: bfloat16 [16384, 7168], P('tp')
Outputs:
- output 1: bfloat16 [4, 512, 7168], P('dp', 'tp'), parts along dimension 0
- output 2: bfloat16 [4, 1024, 512], P('dp'), parts along dimension 0
- output 3: bfloat16 [4, 1024, 64], P('dp'), parts along dimension 0
There are 2 independent parts. The reference program is written for one: setup_inputs(seed, part) draws one part's arguments, and reference() takes and returns one part's arrays. A program takes and returns all parts, laid end to end along the dimension named above; an argument that names none is the same for every part.
All inputs are finite; a program needn't handle non-finite values.
Results may differ from the reference program's by a relative error of at most 0.0138019.
Values are sent between devices in bfloat16 or wider.
A program may use at most 1 GiB of HBM per device.

```python
import jax
import jax.numpy as jnp
from jax import lax

MODEL_DIM = 7168
NUM_HEADS = 128
Q_RANK = 1536
KV_RANK = 512
NOPE_DIM = 128
ROPE_DIM = 64
VALUE_DIM = 128
SEQ_COUNT = 2
CHUNK_LEN = 512
PREFIX_MAX = 512
CACHE_LEN = 1024

HEAD_BLOCK = min(8, NUM_HEADS)


def rms_norm(values, gain_vec):
    inv_rms = lax.rsqrt(jnp.mean(values * values, axis=-1, keepdims=True) + 1e-6)
    return values * inv_rms * gain_vec


def apply_rope(values, cos_tab, sin_tab):
    half_dim = values.shape[-1] // 2
    lower_half = values[..., :half_dim]
    upper_half = values[..., half_dim:]
    return jnp.concatenate([lower_half * cos_tab - upper_half * sin_tab, upper_half * cos_tab + lower_half * sin_tab], axis=-1)


def write_rows(old_rows, new_rows, start_row):
    zero_col = jnp.zeros((), start_row.dtype)
    return lax.dynamic_update_slice(old_rows, new_rows.astype(old_rows.dtype), (start_row, zero_col))


def rope_tables(lengths):
    positions = (lengths[:, None] + jnp.arange(CHUNK_LEN)[None, :]).astype(jnp.float32)
    inv_freq = 10000.0 ** (-2.0 * jnp.arange(ROPE_DIM // 2).astype(jnp.float32) / ROPE_DIM)
    angles = positions[:, :, None] * inv_freq[None, None, :]
    return jnp.cos(angles), jnp.sin(angles)


def normal_draw(key_in, array_shape, std_scale):
    return jax.random.normal(key_in, array_shape, jnp.float32) * std_scale


def setup_inputs(seed: int = 0, part: int = 0) -> dict:
    base_key = jax.random.key(seed)
    part_keys = jax.random.split(jax.random.fold_in(base_key, part), 5)
    weight_keys = jax.random.split(base_key, 9)
    draw_vals = jax.random.randint(part_keys[0], (SEQ_COUNT,), PREFIX_MAX // 4, PREFIX_MAX + 1)
    top_slot = jax.random.randint(part_keys[1], (), 0, SEQ_COUNT)
    lengths = jnp.where(jnp.arange(SEQ_COUNT) == top_slot, PREFIX_MAX, draw_vals).astype(jnp.int32)
    rope_cos, rope_sin = rope_tables(lengths)
    out_scale = (NUM_HEADS * VALUE_DIM) ** -0.5 * (CACHE_LEN / 4.0) ** 0.5
    return {
        "hidden": normal_draw(part_keys[2], (SEQ_COUNT, CHUNK_LEN, MODEL_DIM), 1.0).astype(jnp.bfloat16),
        "lengths": lengths,
        "rope_cos": rope_cos,
        "rope_sin": rope_sin,
        "cache_lat": normal_draw(part_keys[3], (SEQ_COUNT, CACHE_LEN, KV_RANK), 1.0).astype(jnp.bfloat16),
        "cache_pe": normal_draw(part_keys[4], (SEQ_COUNT, CACHE_LEN, ROPE_DIM), 1.0).astype(jnp.bfloat16),
        "norm_in": jax.random.uniform(weight_keys[0], (MODEL_DIM,), jnp.float32, 0.5, 1.5),
        "w_dq": normal_draw(weight_keys[1], (MODEL_DIM, Q_RANK), MODEL_DIM ** -0.5).astype(jnp.bfloat16),
        "norm_q": jax.random.uniform(weight_keys[2], (Q_RANK,), jnp.float32, 0.5, 1.5),
        "w_dkv": normal_draw(weight_keys[3], (MODEL_DIM, KV_RANK + ROPE_DIM), MODEL_DIM ** -0.5).astype(jnp.bfloat16),
        "norm_kv": jax.random.uniform(weight_keys[4], (KV_RANK,), jnp.float32, 0.5, 1.5),
        "w_uq": normal_draw(weight_keys[5], (Q_RANK, NUM_HEADS, NOPE_DIM + ROPE_DIM), Q_RANK ** -0.5).astype(jnp.bfloat16),
        "w_uk": normal_draw(weight_keys[6], (KV_RANK, NUM_HEADS, NOPE_DIM), KV_RANK ** -0.5).astype(jnp.bfloat16),
        "w_uv": normal_draw(weight_keys[7], (KV_RANK, NUM_HEADS, VALUE_DIM), KV_RANK ** -0.5).astype(jnp.bfloat16),
        "w_out": normal_draw(weight_keys[8], (NUM_HEADS * VALUE_DIM, MODEL_DIM), out_scale).astype(jnp.bfloat16),
    }


def reference(hidden, lengths, rope_cos, rope_sin, cache_lat, cache_pe, norm_in, w_dq, norm_q, w_dkv, norm_kv, w_uq, w_uk, w_uv, w_out):
    hidden_f = hidden.astype(jnp.float32)
    normed = rms_norm(hidden_f, norm_in).astype(jnp.bfloat16).reshape(SEQ_COUNT * CHUNK_LEN, MODEL_DIM)
    q_latent = rms_norm(jnp.dot(normed, w_dq, preferred_element_type=jnp.float32), norm_q).astype(jnp.bfloat16)
    kv_proj = jnp.dot(normed, w_dkv, preferred_element_type=jnp.float32).reshape(SEQ_COUNT, CHUNK_LEN, KV_RANK + ROPE_DIM)
    new_lat = rms_norm(kv_proj[..., :KV_RANK], norm_kv).astype(jnp.bfloat16)
    new_pe = apply_rope(kv_proj[..., KV_RANK:], rope_cos, rope_sin).astype(jnp.bfloat16)
    lat_all = jax.vmap(write_rows)(cache_lat, new_lat, lengths)
    pe_all = jax.vmap(write_rows)(cache_pe, new_pe, lengths)
    q_full = jnp.einsum("nc,chd->nhd", q_latent.astype(jnp.float32), w_uq.astype(jnp.float32)).reshape(SEQ_COUNT, CHUNK_LEN, NUM_HEADS, NOPE_DIM + ROPE_DIM)
    q_nope = q_full[..., :NOPE_DIM].astype(jnp.bfloat16)
    q_pe = apply_rope(q_full[..., NOPE_DIM:], rope_cos[:, :, None, :], rope_sin[:, :, None, :]).astype(jnp.bfloat16)
    block_count = NUM_HEADS // HEAD_BLOCK
    uk_blocks = w_uk.reshape(KV_RANK, block_count, HEAD_BLOCK, NOPE_DIM).transpose(1, 0, 2, 3)
    uv_blocks = w_uv.reshape(KV_RANK, block_count, HEAD_BLOCK, VALUE_DIM).transpose(1, 0, 2, 3)
    score_scale = (NOPE_DIM + ROPE_DIM) ** -0.5
    query_pos = jnp.arange(CHUNK_LEN)[:, None]
    key_pos = jnp.arange(CACHE_LEN)[None, :]

    def one_sequence(seq_args):
        qn_seq, qp_seq, lat_seq, pe_seq, length = seq_args
        visible = key_pos < length + query_pos + 1
        qn_blocks = qn_seq.reshape(CHUNK_LEN, block_count, HEAD_BLOCK, NOPE_DIM).transpose(1, 0, 2, 3)
        qp_blocks = qp_seq.reshape(CHUNK_LEN, block_count, HEAD_BLOCK, ROPE_DIM).transpose(1, 0, 2, 3)
        lat_f = lat_seq.astype(jnp.float32)
        pe_f = pe_seq.astype(jnp.float32)

        def one_block(blk_args):
            qn_blk, qp_blk, uk_blk, uv_blk = blk_args
            keys_nope = jnp.einsum("sc,chd->shd", lat_f, uk_blk.astype(jnp.float32)).astype(jnp.bfloat16)
            values_blk = jnp.einsum("sc,chv->shv", lat_f, uv_blk.astype(jnp.float32)).astype(jnp.bfloat16)
            scores = jnp.einsum("thd,shd->hts", qn_blk.astype(jnp.float32), keys_nope.astype(jnp.float32))
            scores = scores + jnp.einsum("thr,sr->hts", qp_blk.astype(jnp.float32), pe_f)
            scores = jnp.where(visible[None], scores * score_scale, -1e30)
            attn_probs = jax.nn.softmax(scores, axis=-1).astype(jnp.bfloat16)
            return jnp.einsum("hts,shv->thv", attn_probs.astype(jnp.float32), values_blk.astype(jnp.float32)).astype(jnp.bfloat16)

        out_blocks = lax.map(one_block, (qn_blocks, qp_blocks, uk_blocks, uv_blocks))
        return out_blocks.transpose(1, 0, 2, 3).reshape(CHUNK_LEN, NUM_HEADS * VALUE_DIM)

    attn_out = lax.map(one_sequence, (q_nope, q_pe, lat_all, pe_all, lengths))
    out_proj = jnp.dot(attn_out.reshape(SEQ_COUNT * CHUNK_LEN, NUM_HEADS * VALUE_DIM), w_out, preferred_element_type=jnp.float32)
    block_out = (out_proj.reshape(SEQ_COUNT, CHUNK_LEN, MODEL_DIM) + hidden_f).astype(jnp.bfloat16)
    return (block_out, lat_all, pe_all)
```

```python
import functools

import jax
import jax.numpy as jnp
from jax import lax
from jax.experimental import pallas as pl
from jax.experimental.pallas import tpu as pltpu
from jax.sharding import PartitionSpec as P

F32 = jnp.float32
BF16 = jnp.bfloat16
NEG = -1e30
LOG2E = 1.4426950408889634
COL_TILE = 512
COL_CHUNKS = 2


def rms_norm(values, gain_vec):
    inv_rms = lax.rsqrt(jnp.mean(values * values, axis=-1, keepdims=True) + 1e-6)
    return values * inv_rms * gain_vec


def apply_rope(values, cos_tab, sin_tab):
    half_dim = values.shape[-1] // 2
    lower_half = values[..., :half_dim]
    upper_half = values[..., half_dim:]
    return jnp.concatenate([lower_half * cos_tab - upper_half * sin_tab, upper_half * cos_tab + lower_half * sin_tab], axis=-1)


def attention_kernel(scal_ref, q_ref, k_old_ref, k_new_ref, v_old_ref, v_new_ref, r_ref, cos_ref, sin_ref, o_ref, *, scale):
    heads, m_rows, _ = q_ref.shape
    nope = k_old_ref.shape[2]
    prefix = k_old_ref.shape[1]
    blk = m_rows
    factor = scale * LOG2E
    cos_tab = cos_ref[...]
    sin_tab = sin_ref[...]
    lane = lax.broadcasted_iota(jnp.int32, (m_rows, nope - 64), 1)
    ones_col = jnp.where(lane == 0, 1.0, 0.0).astype(BF16)
    half = m_rows // 2
    qlane = lax.broadcasted_iota(jnp.int32, (blk, m_rows), 1)
    krow = lax.broadcasted_iota(jnp.int32, (blk, m_rows), 0)
    q_blk0 = scal_ref[0]
    q_blk1 = scal_ref[1]
    base = scal_ref[2] * m_rows
    qpos = jnp.where(qlane < half, q_blk0 * half + qlane, q_blk1 * half + qlane - half) - base
    causal = krow <= qpos

    def body(new_blocks):
        for h in range(heads):
            q_full = q_ref[h]
            q_pe = apply_rope(q_full[:, nope:], cos_tab, sin_tab).astype(BF16)
            q_cat = jnp.concatenate([q_full[:, :nope].astype(BF16), q_pe, ones_col], axis=1)
            scores = []
            for i in range(prefix // blk + new_blocks):
                start = i * blk
                if start < prefix:
                    k_part = k_old_ref[h, start:start + blk, :]
                else:
                    k_part = k_new_ref[h, start - prefix:start - prefix + blk, :]
                k_cat = jnp.concatenate([k_part, r_ref[start:start + blk, :]], axis=1)
                s = lax.dot_general(k_cat, q_cat, (((1,), (1,)), ((), ())), preferred_element_type=F32)
                if i == prefix // blk + new_blocks - 1:
                    s = jnp.where(causal, s, NEG)
                scores.append(s)
            top = functools.reduce(jnp.maximum, scores)
            top = jnp.max(top, axis=0, keepdims=True)
            total = None
            out = None
            for i, s in enumerate(scores):
                start = i * blk
                e = jnp.exp2((s - top) * factor)
                part = jnp.sum(e, axis=0, keepdims=True)
                total = part if total is None else total + part
                if start < prefix:
                    v_part = v_old_ref[h, :, start:start + blk]
                else:
                    v_part = v_new_ref[h, :, start - prefix:start - prefix + blk]
                o_part = jnp.dot(v_part, e.astype(BF16), preferred_element_type=F32)
                out = o_part if out is None else out + o_part
            out = out * (1.0 / total)
            o_ref[:, h * nope:(h + 1) * nope] = out.T.astype(BF16)

    for c in range(v_new_ref.shape[2] // blk):
        @pl.when(scal_ref[2] == c)
        def _(c=c):
            body(c + 1)


def attention(scal, q, k_old, k_new, v_old, v_new, r_cat, cos_tab, sin_tab, scale):
    n_heads, m_rows, q_dim = q.shape
    prefix, nope = k_old.shape[1:]
    n_new = k_new.shape[1]
    hb = 2
    flops = 2 * n_heads * m_rows * (prefix + n_new) * (256 + 128)
    head_blk = lambda *shape: pl.BlockSpec((hb,) + shape, lambda g, s: (g, 0, 0))
    whole = lambda *shape: pl.BlockSpec(shape, lambda g, s: (0, 0))
    return pl.pallas_call(
        functools.partial(attention_kernel, scale=scale),
        out_shape=jax.ShapeDtypeStruct((m_rows, n_heads * nope), BF16),
        grid_spec=pltpu.PrefetchScalarGridSpec(
            num_scalar_prefetch=1,
            grid=(n_heads // hb,),
            in_specs=[
                head_blk(m_rows, q_dim),
                head_blk(prefix, nope),
                head_blk(n_new, nope),
                head_blk(nope, prefix),
                head_blk(nope, n_new),
                whole(*r_cat.shape),
                whole(*cos_tab.shape),
                whole(*sin_tab.shape),
            ],
            out_specs=pl.BlockSpec((m_rows, hb * nope), lambda g, s: (0, g)),
        ),
        compiler_params=pltpu.CompilerParams(dimension_semantics=("arbitrary",)),
        cost_estimate=pl.CostEstimate(flops=flops, bytes_accessed=30_000_000, transcendentals=n_heads * m_rows * (prefix + n_new)),
        name="attention",
    )(scal, q, k_old, k_new, v_old, v_new, r_cat, cos_tab, sin_tab)


def out_proj_kernel(o_ref, w_ref, ya_ref, yb_ref):
    half = ya_ref.shape[0]
    prod = jnp.dot(o_ref[...], w_ref[...], preferred_element_type=F32)
    ya_ref[...] = prod[:half]
    yb_ref[...] = prod[half:]


def out_proj(o, w_out, first, count):
    m_rows, depth = o.shape
    half = m_rows // 2
    tiles = count // COL_TILE
    off = first // COL_TILE
    out = jax.ShapeDtypeStruct((half, count), F32)
    return pl.pallas_call(
        out_proj_kernel,
        out_shape=(out, out),
        grid=(tiles,),
        in_specs=[
            pl.BlockSpec((m_rows, depth), lambda j: (0, 0)),
            pl.BlockSpec((depth, COL_TILE), lambda j: (0, j + off)),
        ],
        out_specs=(pl.BlockSpec((half, COL_TILE), lambda j: (0, j)), pl.BlockSpec((half, COL_TILE), lambda j: (0, j))),
        compiler_params=pltpu.CompilerParams(dimension_semantics=("arbitrary",)),
        cost_estimate=pl.CostEstimate(flops=2 * m_rows * depth * count, bytes_accessed=depth * count * 2 + m_rows * count * 4, transcendentals=0),
        name="out_proj",
    )(o, w_out)


def solution(mesh):
    tp = mesh.shape["tp"]
    to_partner = [(i, i ^ 1) for i in range(tp)]
    to_chip = [(i, i ^ 2) for i in range(tp)]

    def partner(value):
        return lax.ppermute(value, "tp", to_partner)

    def other_chip(value):
        return lax.ppermute(value, "tp", to_chip)

    def local_step(hidden, lengths, rope_cos, rope_sin, cache_lat, cache_pe, norm_in, w_dq, norm_q, w_dkv, norm_kv, w_uq, w_uk, w_uv, w_out):
        me = lax.axis_index("tp")
        n_seq, n_tok, model_dim = hidden.shape
        kv_rank, n_heads, nope = w_uk.shape
        rope_dim = cache_pe.shape[2]
        n_new = rope_cos.shape[1]
        prefix = cache_lat.shape[1] - n_new
        q_rank = w_dq.shape[1]
        scale = (nope + rope_dim) ** -0.5

        normed = rms_norm(hidden.astype(F32), norm_in).astype(BF16).reshape(n_seq * n_tok, model_dim)
        kv_proj = jnp.dot(normed, w_dkv, preferred_element_type=F32).reshape(n_seq, n_tok, kv_rank + rope_dim)
        my_cos = lax.dynamic_slice_in_dim(rope_cos, me * n_tok, n_tok, axis=1)
        my_sin = lax.dynamic_slice_in_dim(rope_sin, me * n_tok, n_tok, axis=1)
        my_lat = rms_norm(kv_proj[..., :kv_rank], norm_kv).astype(BF16)
        my_pe = apply_rope(kv_proj[..., kv_rank:], my_cos, my_sin).astype(BF16)
        my_kv = jnp.concatenate([my_lat, my_pe], axis=-1)
        my_q = rms_norm(jnp.dot(normed, w_dq, preferred_element_type=F32), norm_q).astype(BF16).reshape(n_seq, n_tok, q_rank)

        def gather(value):
            far = other_chip(value)
            near = partner(value)
            return [value, near, far, partner(far)]

        kv_rel = jnp.stack(gather(my_kv))
        kv_true = jnp.concatenate([lax.dynamic_index_in_dim(kv_rel, me ^ j, keepdims=False) for j in range(tp)], axis=1)
        lat_new = kv_true[..., :kv_rank]
        pe_new = kv_true[..., kv_rank:]
        q_rel = [gather(my_q[b]) for b in range(n_seq)]

        def project(lat):
            keys = jnp.einsum("sc,chd->hsd", lat, w_uk, preferred_element_type=F32).astype(BF16)
            values = jnp.einsum("chv,sc->hvs", w_uv, lat, preferred_element_type=F32).astype(BF16)
            return keys, values

        row = jnp.arange(prefix)
        alive = row[None, :] < lengths[:, None]
        old_lat = jnp.where(alive[..., None], cache_lat[:, :prefix], 0)
        old_pe = jnp.where(alive[..., None], cache_pe[:, :prefix], 0)
        kv_old = [project(old_lat[b]) for b in range(n_seq)]
        kv_new = [project(lat_new[b]) for b in range(n_seq)]
        bias = jnp.where(alive, 0.0, NEG).astype(BF16)[..., None]
        pad_old = jnp.zeros((n_seq, prefix, nope - rope_dim - 1), BF16)
        pad_new = jnp.zeros((n_seq, n_new, nope - rope_dim), BF16)
        r_cat = jnp.concatenate([
            jnp.concatenate([old_pe, bias, pad_old], axis=-1),
            jnp.concatenate([pe_new, pad_new], axis=-1)], axis=1)

        def attend(rel, b):
            blocks = (me ^ rel, me ^ (rel + 1))
            scal = jnp.stack([blocks[0], blocks[1], blocks[0] // 2]).astype(jnp.int32)
            q_lat = jnp.concatenate([q_rel[b][rel], q_rel[b][rel + 1]], axis=0)
            q = jnp.einsum("tq,qhd->htd", q_lat, w_uq, preferred_element_type=F32)
            cut = lambda tab: jnp.concatenate([lax.dynamic_slice_in_dim(tab[b], k * n_tok, n_tok, axis=0) for k in blocks], axis=0)
            return attention(scal, q, kv_old[b][0], kv_new[b][0], kv_old[b][1], kv_new[b][1], r_cat[b], cut(rope_cos), cut(rope_sin), scale)

        width = model_dim // COL_CHUNKS
        arrived = []
        for b in range(n_seq):
            o = attend(2, b)
            cols = []
            for j in range(COL_CHUNKS):
                near_part, far_part = out_proj(o, w_out, j * width, width)
                cols.append(other_chip(near_part + partner(far_part)))
            arrived.append(cols)
        result = []
        for b in range(n_seq):
            o = attend(0, b)
            own_part, partner_part = out_proj(o, w_out, 0, model_dim)
            base = own_part + partner(partner_part) + hidden[b].astype(F32)
            result.append((base + jnp.concatenate(arrived[b], axis=1)).astype(BF16))
        out = jnp.stack(result)
        lat_all = jnp.stack([lax.dynamic_update_slice(cache_lat[b], lat_new[b], (lengths[b], 0)) for b in range(n_seq)])
        pe_all = jnp.stack([lax.dynamic_update_slice(cache_pe[b], pe_new[b], (lengths[b], 0)) for b in range(n_seq)])
        return out, lat_all, pe_all

    spec_tok = P("dp", "tp", None)
    spec_len = P("dp")
    spec_seq = P("dp", None, None)
    spec_vec = P(None)
    spec_mat = P(None, None)
    spec_head = P(None, "tp", None)
    spec_rows = P("tp", None)
    in_specs = (spec_tok, spec_len, spec_seq, spec_seq, spec_seq, spec_seq, spec_vec, spec_mat, spec_vec, spec_mat, spec_vec, spec_head, spec_head, spec_head, spec_rows)
    return jax.shard_map(local_step, mesh=mesh, in_specs=in_specs, out_specs=(spec_tok, spec_seq, spec_seq), check_vma=False)
```

```python
import functools

import jax
import jax.numpy as jnp
from jax import lax
from jax.experimental import pallas as pl
from jax.experimental.pallas import tpu as pltpu
from jax.sharding import PartitionSpec as P


F32 = jnp.float32
BF16 = jnp.bfloat16
NEG = -1e30
LOG2E = 1.4426950408889634
COL_TILE = 512
COL_CHUNKS = 2
HEADS_PER_STEP = 2


def rms_norm(values, gain_vec):
    inv_rms = lax.rsqrt(jnp.mean(values * values, axis=-1, keepdims=True) + 1e-6)
    return values * inv_rms * gain_vec


def apply_rope(values, cos_tab, sin_tab):
    half_dim = values.shape[-1] // 2
    lower_half = values[..., :half_dim]
    upper_half = values[..., half_dim:]
    return jnp.concatenate([lower_half * cos_tab - upper_half * sin_tab, upper_half * cos_tab + lower_half * sin_tab], axis=-1)


def attention_kernel(scal_ref, q_ref, k_old_ref, k_new_ref, v_old_ref, v_new_ref, r_ref, cos_ref, sin_ref, o_ref, *, scale):
    heads, _, m_rows = q_ref.shape
    nope = k_old_ref.shape[2]
    prefix = k_old_ref.shape[1]
    rope_half = cos_ref.shape[0]
    blk = m_rows
    factor = scale * LOG2E
    cos_tab = cos_ref[...]
    sin_tab = sin_ref[...]
    pad_row = lax.broadcasted_iota(jnp.int32, (nope - 2 * rope_half, m_rows), 0)
    ones_row = jnp.where(pad_row == 0, 1.0, 0.0).astype(BF16)
    half = m_rows // 2
    qlane = lax.broadcasted_iota(jnp.int32, (blk, m_rows), 1)
    krow = lax.broadcasted_iota(jnp.int32, (blk, m_rows), 0)
    q_blk0 = scal_ref[0]
    q_blk1 = scal_ref[1]
    base = scal_ref[2] * m_rows
    qpos = jnp.where(qlane < half, q_blk0 * half + qlane, q_blk1 * half + qlane - half) - base
    causal = krow <= qpos

    def body(new_blocks):
        for h in range(heads):
            low = q_ref[h, nope:nope + rope_half, :]
            high = q_ref[h, nope + rope_half:, :]
            q_cat = jnp.concatenate([
                q_ref[h, :nope, :].astype(BF16),
                (low * cos_tab - high * sin_tab).astype(BF16),
                (high * cos_tab + low * sin_tab).astype(BF16),
                ones_row], axis=0)
            scores = []
            for i in range(prefix // blk + new_blocks):
                start = i * blk
                if start < prefix:
                    k_part = k_old_ref[h, start:start + blk, :]
                else:
                    k_part = k_new_ref[h, start - prefix:start - prefix + blk, :]
                k_cat = jnp.concatenate([k_part, r_ref[start:start + blk, :]], axis=1)
                s = jnp.dot(k_cat, q_cat, preferred_element_type=F32)
                if i == prefix // blk + new_blocks - 1:
                    s = jnp.where(causal, s, NEG)
                scores.append(s)
            top = functools.reduce(jnp.maximum, scores)
            top = jnp.max(top, axis=0, keepdims=True)
            total = None
            out = None
            for i, s in enumerate(scores):
                start = i * blk
                e = jnp.exp2((s - top) * factor)
                part = jnp.sum(e, axis=0, keepdims=True)
                total = part if total is None else total + part
                if start < prefix:
                    v_part = v_old_ref[h, :, start:start + blk]
                else:
                    v_part = v_new_ref[h, :, start - prefix:start - prefix + blk]
                o_part = jnp.dot(v_part, e.astype(BF16), preferred_element_type=F32)
                out = o_part if out is None else out + o_part
            out = out * (1.0 / total)
            o_ref[:, h * nope:(h + 1) * nope] = out.T.astype(BF16)

    for c in range(v_new_ref.shape[2] // blk):
        @pl.when(scal_ref[2] == c)
        def _(c=c):
            body(c + 1)


def attention(scal, q, q_tile, k_old, k_new, v_old, v_new, r_cat, cos_tab, sin_tab, scale):
    n_heads, q_dim, _ = q.shape
    m_rows = cos_tab.shape[1]
    prefix, nope = k_old.shape[1:]
    n_new = k_new.shape[1]
    hb = HEADS_PER_STEP
    flops = 2 * n_heads * m_rows * (prefix + n_new) * (256 + 128)
    head_blk = lambda *shape: pl.BlockSpec((hb,) + shape, lambda g, s: (g, 0, 0))
    whole = lambda *shape: pl.BlockSpec(shape, lambda g, s: (0, 0))
    return pl.pallas_call(
        functools.partial(attention_kernel, scale=scale),
        out_shape=jax.ShapeDtypeStruct((m_rows, n_heads * nope), BF16),
        grid_spec=pltpu.PrefetchScalarGridSpec(
            num_scalar_prefetch=1,
            grid=(n_heads // hb,),
            in_specs=[
                pl.BlockSpec((hb, q_dim, m_rows), lambda g, s: (g, 0, q_tile)),
                head_blk(prefix, nope),
                head_blk(n_new, nope),
                head_blk(nope, prefix),
                head_blk(nope, n_new),
                whole(*r_cat.shape),
                whole(*cos_tab.shape),
                whole(*sin_tab.shape),
            ],
            out_specs=pl.BlockSpec((m_rows, hb * nope), lambda g, s: (0, g)),
        ),
        compiler_params=pltpu.CompilerParams(dimension_semantics=("arbitrary",)),
        cost_estimate=pl.CostEstimate(flops=flops, bytes_accessed=30_000_000, transcendentals=n_heads * m_rows * (prefix + n_new)),
        name="attention",
    )(scal, q, k_old, k_new, v_old, v_new, r_cat, cos_tab, sin_tab)


def out_proj_kernel(o_ref, w_ref, ya_ref, yb_ref):
    half = ya_ref.shape[0]
    prod = jnp.dot(o_ref[...], w_ref[...], preferred_element_type=F32)
    ya_ref[...] = prod[:half]
    yb_ref[...] = prod[half:]


def out_proj(o, w_out, first, count):
    m_rows, depth = o.shape
    half = m_rows // 2
    tiles = count // COL_TILE
    off = first // COL_TILE
    out = jax.ShapeDtypeStruct((half, count), F32)
    return pl.pallas_call(
        out_proj_kernel,
        out_shape=(out, out),
        grid=(tiles,),
        in_specs=[
            pl.BlockSpec((m_rows, depth), lambda j: (0, 0)),
            pl.BlockSpec((depth, COL_TILE), lambda j: (0, j + off)),
        ],
        out_specs=(pl.BlockSpec((half, COL_TILE), lambda j: (0, j)), pl.BlockSpec((half, COL_TILE), lambda j: (0, j))),
        compiler_params=pltpu.CompilerParams(dimension_semantics=("arbitrary",)),
        cost_estimate=pl.CostEstimate(flops=2 * m_rows * depth * count, bytes_accessed=depth * count * 2 + m_rows * count * 4, transcendentals=0),
        name="out_proj",
    )(o, w_out)


def solution(mesh):
    tp = mesh.shape["tp"]
    to_partner = [(i, i ^ 1) for i in range(tp)]
    to_chip = [(i, i ^ 2) for i in range(tp)]

    def partner(value):
        return lax.ppermute(value, "tp", to_partner)

    def other_chip(value):
        return lax.ppermute(value, "tp", to_chip)

    def step(hidden, lengths, rope_cos, rope_sin, cache_lat, cache_pe, norm_in, w_dq, norm_q, w_dkv, norm_kv, w_uq, w_uk, w_uv, w_out):
        me = lax.axis_index("tp")
        n_seq, n_tok, model_dim = hidden.shape
        kv_rank, _, nope = w_uk.shape
        rope_dim = cache_pe.shape[2]
        n_new = rope_cos.shape[1]
        prefix = cache_lat.shape[1] - n_new
        q_rank = w_dq.shape[1]
        scale = (nope + rope_dim) ** -0.5

        normed = rms_norm(hidden.astype(F32), norm_in).astype(BF16).reshape(n_seq * n_tok, model_dim)
        kv_proj = jnp.dot(normed, w_dkv, preferred_element_type=F32).reshape(n_seq, n_tok, kv_rank + rope_dim)
        my_cos = lax.dynamic_slice_in_dim(rope_cos, me * n_tok, n_tok, axis=1)
        my_sin = lax.dynamic_slice_in_dim(rope_sin, me * n_tok, n_tok, axis=1)
        my_lat = rms_norm(kv_proj[..., :kv_rank], norm_kv).astype(BF16)
        my_pe = apply_rope(kv_proj[..., kv_rank:], my_cos, my_sin).astype(BF16)
        my_kv = jnp.concatenate([my_lat, my_pe], axis=-1)
        my_q = rms_norm(jnp.dot(normed, w_dq, preferred_element_type=F32), norm_q).astype(BF16).reshape(n_seq, n_tok, q_rank)

        def gather(value):
            far = other_chip(value)
            near = partner(value)
            return [value, near, far, partner(far)]

        kv_rel = jnp.stack(gather(my_kv))
        kv_true = jnp.concatenate([lax.dynamic_index_in_dim(kv_rel, me ^ j, keepdims=False) for j in range(tp)], axis=1)
        lat_new = kv_true[..., :kv_rank]
        pe_new = kv_true[..., kv_rank:]
        q_rel = [gather(my_q[b]) for b in range(n_seq)]

        def project(lat):
            keys = jnp.einsum("sc,chd->hsd", lat, w_uk, preferred_element_type=F32).astype(BF16)
            values = jnp.einsum("chv,sc->hvs", w_uv, lat, preferred_element_type=F32).astype(BF16)
            return keys, values

        row = jnp.arange(prefix)
        alive = row[None, :] < lengths[:, None]
        old_lat = jnp.where(alive[..., None], cache_lat[:, :prefix], 0)
        old_pe = jnp.where(alive[..., None], cache_pe[:, :prefix], 0)
        kv_old = [project(old_lat[b]) for b in range(n_seq)]
        kv_new = [project(lat_new[b]) for b in range(n_seq)]
        bias = jnp.where(alive, 0.0, NEG).astype(BF16)[..., None]
        pad_old = jnp.zeros((n_seq, prefix, nope - rope_dim - 1), BF16)
        pad_new = jnp.zeros((n_seq, n_new, nope - rope_dim), BF16)
        r_cat = jnp.concatenate([
            jnp.concatenate([old_pe, bias, pad_old], axis=-1),
            jnp.concatenate([pe_new, pad_new], axis=-1)], axis=1)

        def queries(q_lat):
            return jnp.einsum("qhd,tq->hdt", w_uq, q_lat, preferred_element_type=F32)

        def attend(rel, b, q, q_tile):
            blocks = (me ^ rel, me ^ (rel + 1))
            scal = jnp.stack([blocks[0], blocks[1], blocks[0] // 2]).astype(jnp.int32)
            cut = lambda tab: jnp.concatenate([lax.dynamic_slice_in_dim(tab[b], k * n_tok, n_tok, axis=0) for k in blocks], axis=0).T
            return attention(scal, q, q_tile, kv_old[b][0], kv_new[b][0], kv_old[b][1], kv_new[b][1], r_cat[b], cut(rope_cos), cut(rope_sin), scale)

        def after(value, *deps):
            return lax.optimization_barrier((value,) + deps)[0]

        width = model_dim // COL_CHUNKS
        arrived = [[None] * COL_CHUNKS for _ in range(n_seq)]
        pending = []

        def send_one():
            b, j, near_part, came = pending.pop(0)
            summed = near_part + came
            arrived[b][j] = other_chip(summed)
            return summed

        near_part = None
        for b in range(n_seq):
            q_lat = jnp.concatenate(q_rel[b][2:], axis=0)
            if near_part is not None:
                q_lat = after(q_lat, near_part)
            q = queries(q_lat)
            if pending:
                q = after(q, send_one())
            o = attend(2, b, q, 0)
            for j in range(COL_CHUNKS):
                if len(pending) > 1 - (j == 0):
                    o = after(o, send_one())
                near_part, far_part = out_proj(o, w_out, j * width, width)
                pending.append((b, j, near_part, partner(far_part)))
        q_lat = jnp.concatenate([q_rel[b][k] for b in range(n_seq) for k in (0, 1)], axis=0)
        q_lat = after(q_lat, near_part)
        q_own = queries(q_lat)
        while pending:
            q_own = after(q_own, send_one())
        result = []
        for b in range(n_seq):
            o = attend(0, b, q_own, b)
            own_part, partner_part = out_proj(o, w_out, 0, model_dim)
            base = own_part + partner(partner_part) + hidden[b].astype(F32)
            result.append((base + jnp.concatenate(arrived[b], axis=1)).astype(BF16))
        out = jnp.stack(result)
        lat_all = jnp.stack([lax.dynamic_update_slice(cache_lat[b], lat_new[b], (lengths[b], 0)) for b in range(n_seq)])
        pe_all = jnp.stack([lax.dynamic_update_slice(cache_pe[b], pe_new[b], (lengths[b], 0)) for b in range(n_seq)])
        return out, lat_all, pe_all

    spec_tok = P("dp", "tp", None)
    spec_len = P("dp")
    spec_seq = P("dp", None, None)
    spec_vec = P(None)
    spec_mat = P(None, None)
    spec_head = P(None, "tp", None)
    spec_rows = P("tp", None)
    in_specs = (spec_tok, spec_len, spec_seq, spec_seq, spec_seq, spec_seq, spec_vec, spec_mat, spec_vec, spec_mat, spec_vec, spec_head, spec_head, spec_head, spec_rows)
    return jax.shard_map(step, mesh=mesh, in_specs=in_specs, out_specs=(spec_tok, spec_seq, spec_seq), check_vma=False)
```

```python
import functools

import jax
import jax.numpy as jnp
from jax import lax
from jax.experimental import pallas as pl
from jax.experimental.pallas import tpu as pltpu
from jax.sharding import PartitionSpec as P


F32 = jnp.float32
BF16 = jnp.bfloat16
NEG = -1e30
LOG2E = 1.4426950408889634
COL_TILE = 512
COL_CHUNKS = 2
HEADS_PER_STEP = 2
SLOTS = 4
W_SLOTS = 4


def rms_norm(values, gain_vec):
    inv_rms = lax.rsqrt(jnp.mean(values * values, axis=-1, keepdims=True) + 1e-6)
    return values * inv_rms * gain_vec


def apply_rope(values, cos_tab, sin_tab):
    half_dim = values.shape[-1] // 2
    lower_half = values[..., :half_dim]
    upper_half = values[..., half_dim:]
    return jnp.concatenate([lower_half * cos_tab - upper_half * sin_tab, upper_half * cos_tab + lower_half * sin_tab], axis=-1)


def attention_kernel(scal_ref, q_lat_ref, r_ref, cos_ref, sin_ref, w_hbm, k_old_hbm, k_new_hbm, v_old_hbm, v_new_hbm, o_ref,
                     w_buf, k_buf, v_buf, q_lat_t, scores_a, scores_b, top_a, top_b, sems, *, scale):
    step = pl.program_id(0)
    n_steps = pl.num_programs(0)
    m_rows = q_lat_ref.shape[0]
    nope = k_buf.shape[3]
    prefix = k_old_hbm.shape[1]
    rope_half = cos_ref.shape[0]
    blk = m_rows
    half = m_rows // 2
    factor = scale * LOG2E

    def copies(g, slot):
        heads = pl.ds(g * HEADS_PER_STEP, HEADS_PER_STEP)
        pairs = (
            (w_hbm.at[heads], w_buf.at[slot]),
            (k_old_hbm.at[heads], k_buf.at[slot, :, :prefix]),
            (k_new_hbm.at[heads], k_buf.at[slot, :, prefix:]),
            (v_old_hbm.at[heads], v_buf.at[slot, :, :, :prefix]),
            (v_new_hbm.at[heads], v_buf.at[slot, :, :, prefix:]),
        )
        return [pltpu.make_async_copy(src, dst, sems.at[slot, i]) for i, (src, dst) in enumerate(pairs)]

    def fetch(g, slot):
        for copy in copies(g, slot):
            copy.start()

    def arrive(g, slot):
        for copy in copies(g, slot):
            copy.wait()

    def body(new_blocks):
        n_blk = prefix // blk + new_blocks

        def score(slot, h, scores, top):
            q_t = jnp.dot(w_buf[slot, h], q_lat_t[...], preferred_element_type=F32)
            low = q_t[nope:nope + rope_half]
            high = q_t[nope + rope_half:]
            pad_row = lax.broadcasted_iota(jnp.int32, (nope - 2 * rope_half, m_rows), 0)
            q_cat = jnp.concatenate([
                q_t[:nope].astype(BF16),
                (low * cos_ref[...] - high * sin_ref[...]).astype(BF16),
                (high * cos_ref[...] + low * sin_ref[...]).astype(BF16),
                jnp.where(pad_row == 0, 1.0, 0.0).astype(BF16)], axis=0)
            best = None
            for i in range(n_blk):
                rows = slice(i * blk, (i + 1) * blk)
                k_cat = jnp.concatenate([k_buf[slot, h, rows, :], r_ref[rows, :]], axis=1)
                s = jnp.dot(k_cat, q_cat, preferred_element_type=F32)
                if i == n_blk - 1:
                    qlane = lax.broadcasted_iota(jnp.int32, (blk, m_rows), 1)
                    krow = lax.broadcasted_iota(jnp.int32, (blk, m_rows), 0)
                    qpos = jnp.where(qlane < half, scal_ref[0] * half + qlane, scal_ref[1] * half + qlane - half)
                    s = jnp.where(krow <= qpos - scal_ref[2] * m_rows, s, NEG)
                scores[rows, :] = s
                top_i = jnp.max(s, axis=0, keepdims=True)
                best = top_i if best is None else jnp.maximum(best, top_i)
            top[...] = best

        def finish(slot, h, scores, top):
            best = top[...]
            total = None
            out = None
            for i in range(n_blk):
                rows = slice(i * blk, (i + 1) * blk)
                e = jnp.exp2((scores[rows, :] - best) * factor)
                part = jnp.sum(e, axis=0, keepdims=True)
                total = part if total is None else total + part
                o_part = jnp.dot(v_buf[slot, h, :, rows], e.astype(BF16), preferred_element_type=F32)
                out = o_part if out is None else out + o_part
            out = out * (1.0 / total)
            o_ref[:, h * nope:(h + 1) * nope] = out.T.astype(BF16)

        @pl.when(step == 0)
        def _():
            for g in range(SLOTS):
                fetch(g, g)
            q_lat_t[...] = q_lat_ref[...].T
            arrive(0, 0)
            score(0, 0, scores_a, top_a)

        slot = lax.rem(step, SLOTS)
        following = jnp.minimum(step + 1, n_steps - 1)
        next_slot = lax.rem(following, SLOTS)
        score(slot, 1, scores_b, top_b)
        finish(slot, 0, scores_a, top_a)

        @pl.when(step + 1 < n_steps)
        def _():
            arrive(step + 1, next_slot)

        score(next_slot, 0, scores_a, top_a)
        finish(slot, 1, scores_b, top_b)

        @pl.when(step + SLOTS < n_steps)
        def _():
            fetch(step + SLOTS, slot)

    for c in range((k_buf.shape[2] - prefix) // blk):
        @pl.when(scal_ref[2] == c)
        def _(c=c):
            body(c + 1)


def attention(scal, q_lat, w_t, k_old, k_new, v_old, v_new, r_cat, cos_tab, sin_tab, scale):
    n_heads, q_dim, q_rank = w_t.shape
    m_rows = q_lat.shape[0]
    prefix, nope = k_old.shape[1:]
    n_keys = prefix + k_new.shape[1]
    hb = HEADS_PER_STEP
    flops = 2 * n_heads * m_rows * (n_keys * (256 + 128) + q_dim * q_rank)
    whole = lambda arr: pl.BlockSpec(arr.shape, lambda g, s: (0, 0))
    raw = pl.BlockSpec(memory_space=pl.ANY)
    return pl.pallas_call(
        functools.partial(attention_kernel, scale=scale),
        out_shape=jax.ShapeDtypeStruct((m_rows, n_heads * nope), BF16),
        grid_spec=pltpu.PrefetchScalarGridSpec(
            num_scalar_prefetch=1,
            grid=(n_heads // hb,),
            in_specs=[whole(q_lat), whole(r_cat), whole(cos_tab), whole(sin_tab), raw, raw, raw, raw, raw],
            out_specs=pl.BlockSpec((m_rows, hb * nope), lambda g, s: (0, g)),
            scratch_shapes=[
                pltpu.VMEM((SLOTS, hb, q_dim, q_rank), BF16),
                pltpu.VMEM((SLOTS, hb, n_keys, nope), BF16),
                pltpu.VMEM((SLOTS, hb, nope, n_keys), BF16),
                pltpu.VMEM((q_rank, m_rows), BF16),
                pltpu.VMEM((n_keys, m_rows), F32),
                pltpu.VMEM((n_keys, m_rows), F32),
                pltpu.VMEM((1, m_rows), F32),
                pltpu.VMEM((1, m_rows), F32),
                pltpu.SemaphoreType.DMA((SLOTS, 5)),
            ],
        ),
        compiler_params=pltpu.CompilerParams(dimension_semantics=("arbitrary",)),
        cost_estimate=pl.CostEstimate(flops=flops, bytes_accessed=38_000_000, transcendentals=n_heads * m_rows * n_keys),
        name="attention",
    )(scal, q_lat, r_cat, cos_tab, sin_tab, w_t, k_old, k_new, v_old, v_new)


def out_proj_kernel(*refs, n_in, first):
    o_hbm = refs[:n_in]
    w_hbm, near_ref, far_ref, o_buf, w_buf, o_sems, w_sems = refs[n_in:]
    j = pl.program_id(0)
    tiles = pl.num_programs(0)
    slots = w_buf.shape[0]
    half = o_buf.shape[1] // 2

    def weights(tile, slot):
        col = pl.multiple_of((tile + first) * COL_TILE, COL_TILE)
        return pltpu.make_async_copy(w_hbm.at[:, pl.ds(col, COL_TILE)], w_buf.at[slot], w_sems.at[slot])

    @pl.when(j == 0)
    def _():
        weights(0, 0).start()
        loads = [pltpu.make_async_copy(o_hbm[i], o_buf.at[i], o_sems.at[i]) for i in range(n_in)]
        for load in loads:
            load.start()
        for slot in range(1, slots):
            weights(slot, slot).start()
        for load in loads:
            load.wait()

    slot = lax.rem(j, slots)
    weights(j, slot).wait()
    for i in range(n_in):
        prod = jnp.dot(o_buf[i], w_buf[slot], preferred_element_type=F32)
        near_ref[i * half:(i + 1) * half, :] = prod[:half]
        far_ref[i * half:(i + 1) * half, :] = prod[half:]

    @pl.when(j + slots < tiles)
    def _():
        weights(j + slots, slot).start()


def out_proj(o_list, w_out, first, count):
    m_rows, depth = o_list[0].shape
    n_in = len(o_list)
    half = m_rows // 2
    tiles = count // COL_TILE
    out = jax.ShapeDtypeStruct((n_in * half, count), F32)
    raw = pl.BlockSpec(memory_space=pl.ANY)
    out_spec = pl.BlockSpec((n_in * half, COL_TILE), lambda j: (0, j))
    return pl.pallas_call(
        functools.partial(out_proj_kernel, n_in=n_in, first=first // COL_TILE),
        out_shape=(out, out),
        grid=(tiles,),
        in_specs=[raw] * (n_in + 1),
        out_specs=(out_spec, out_spec),
        scratch_shapes=[
            pltpu.VMEM((n_in, m_rows, depth), BF16),
            pltpu.VMEM((W_SLOTS, depth, COL_TILE), BF16),
            pltpu.SemaphoreType.DMA((n_in,)),
            pltpu.SemaphoreType.DMA((W_SLOTS,)),
        ],
        compiler_params=pltpu.CompilerParams(dimension_semantics=("arbitrary",)),
        cost_estimate=pl.CostEstimate(flops=2 * n_in * m_rows * depth * count, bytes_accessed=depth * count * 2 + n_in * m_rows * count * 4, transcendentals=0),
        name="out_proj",
    )(*o_list, w_out)


def solution(mesh):
    tp = mesh.shape["tp"]
    to_partner = [(i, i ^ 1) for i in range(tp)]
    to_chip = [(i, i ^ 2) for i in range(tp)]

    def partner(value):
        return lax.ppermute(value, "tp", to_partner)

    def other_chip(value):
        return lax.ppermute(value, "tp", to_chip)

    def step(hidden, lengths, rope_cos, rope_sin, cache_lat, cache_pe, norm_in, w_dq, norm_q, w_dkv, norm_kv, w_uq, w_uk, w_uv, w_out):
        me = lax.axis_index("tp")
        n_seq, n_tok, model_dim = hidden.shape
        kv_rank, _, nope = w_uk.shape
        rope_dim = cache_pe.shape[2]
        n_new = rope_cos.shape[1]
        prefix = cache_lat.shape[1] - n_new
        q_rank = w_dq.shape[1]
        scale = (nope + rope_dim) ** -0.5

        normed = rms_norm(hidden.astype(F32), norm_in).astype(BF16).reshape(n_seq * n_tok, model_dim)
        kv_proj = jnp.dot(normed, w_dkv, preferred_element_type=F32).reshape(n_seq, n_tok, kv_rank + rope_dim)
        my_cos = lax.dynamic_slice_in_dim(rope_cos, me * n_tok, n_tok, axis=1)
        my_sin = lax.dynamic_slice_in_dim(rope_sin, me * n_tok, n_tok, axis=1)
        my_lat = rms_norm(kv_proj[..., :kv_rank], norm_kv).astype(BF16)
        my_pe = apply_rope(kv_proj[..., kv_rank:], my_cos, my_sin).astype(BF16)
        my_kv = jnp.concatenate([my_lat, my_pe], axis=-1)
        my_q = rms_norm(jnp.dot(normed, w_dq, preferred_element_type=F32), norm_q).astype(BF16).reshape(n_seq, n_tok, q_rank)

        def gather(value):
            far = other_chip(value)
            near = partner(value)
            return [value, near, far, partner(far)]

        kv_rel = jnp.stack(gather(my_kv))
        kv_true = jnp.concatenate([lax.dynamic_index_in_dim(kv_rel, me ^ j, keepdims=False) for j in range(tp)], axis=1)
        lat_new = kv_true[..., :kv_rank]
        pe_new = kv_true[..., kv_rank:]
        q_rel = [gather(my_q[b]) for b in range(n_seq)]

        def project(lat):
            keys = jnp.einsum("sc,chd->hsd", lat, w_uk, preferred_element_type=F32).astype(BF16)
            values = jnp.einsum("chv,sc->hvs", w_uv, lat, preferred_element_type=F32).astype(BF16)
            return keys, values

        row = jnp.arange(prefix)
        alive = row[None, :] < lengths[:, None]
        old_lat = jnp.where(alive[..., None], cache_lat[:, :prefix], 0)
        old_pe = jnp.where(alive[..., None], cache_pe[:, :prefix], 0)
        kv_old = [project(old_lat[b]) for b in range(n_seq)]
        kv_new = [project(lat_new[b]) for b in range(n_seq)]
        bias = jnp.where(alive, 0.0, NEG).astype(BF16)[..., None]
        pad_old = jnp.zeros((n_seq, prefix, nope - rope_dim - 1), BF16)
        pad_new = jnp.zeros((n_seq, n_new, nope - rope_dim), BF16)
        r_cat = jnp.concatenate([
            jnp.concatenate([old_pe, bias, pad_old], axis=-1),
            jnp.concatenate([pe_new, pad_new], axis=-1)], axis=1)

        w_t = w_uq.transpose(1, 2, 0)

        def attend(rel, b, q_lat):
            blocks = (me ^ rel, me ^ (rel + 1))
            scal = jnp.stack([blocks[0], blocks[1], blocks[0] // 2]).astype(jnp.int32)
            cut = lambda tab: jnp.concatenate([lax.dynamic_slice_in_dim(tab[b], k * n_tok, n_tok, axis=0) for k in blocks], axis=0).T
            return attention(scal, q_lat, w_t, kv_old[b][0], kv_new[b][0], kv_old[b][1], kv_new[b][1], r_cat[b], cut(rope_cos), cut(rope_sin), scale)

        def after(value, *deps):
            return lax.optimization_barrier((value,) + deps)[0]

        width = model_dim // COL_CHUNKS
        arrived = [[None] * COL_CHUNKS for _ in range(n_seq)]
        pending = []

        def send_one():
            b, j, near_part, came = pending.pop(0)
            summed = near_part + came
            arrived[b][j] = other_chip(summed)
            return summed

        near_part = None
        for b in range(n_seq):
            q_lat = jnp.concatenate(q_rel[b][2:], axis=0)
            if near_part is not None:
                q_lat = after(q_lat, near_part, send_one())
            o = attend(2, b, q_lat)
            for j in range(COL_CHUNKS):
                if len(pending) > 1 - (j == 0):
                    o = after(o, send_one())
                near_part, far_part = out_proj([o], w_out, j * width, width)
                pending.append((b, j, near_part, partner(far_part)))
        dep = (near_part, send_one())
        o_own = []
        for b in range(n_seq):
            q_lat = after(jnp.concatenate(q_rel[b][:2], axis=0), *dep)
            o_own.append(attend(0, b, q_lat))
            dep = (o_own[-1],) + ((send_one(),) if pending else ())
        cols = []
        flat = hidden.reshape(n_seq * n_tok, model_dim)
        for j in range(COL_CHUNKS):
            own_part, partner_part = out_proj([after(o_own[0], *dep), o_own[1]], w_out, j * width, width)
            dep = (own_part,)
            base = own_part + partner(partner_part) + flat[:, j * width:(j + 1) * width].astype(F32)
            cols.append(base + jnp.concatenate([arrived[b][j] for b in range(n_seq)], axis=0))
        out = jnp.concatenate(cols, axis=1).astype(BF16).reshape(hidden.shape)
        lat_all = jnp.stack([lax.dynamic_update_slice(cache_lat[b], lat_new[b], (lengths[b], 0)) for b in range(n_seq)])
        pe_all = jnp.stack([lax.dynamic_update_slice(cache_pe[b], pe_new[b], (lengths[b], 0)) for b in range(n_seq)])
        return out, lat_all, pe_all

    spec_tok = P("dp", "tp", None)
    spec_len = P("dp")
    spec_seq = P("dp", None, None)
    spec_vec = P(None)
    spec_mat = P(None, None)
    spec_head = P(None, "tp", None)
    spec_rows = P("tp", None)
    in_specs = (spec_tok, spec_len, spec_seq, spec_seq, spec_seq, spec_seq, spec_vec, spec_mat, spec_vec, spec_mat, spec_vec, spec_head, spec_head, spec_head, spec_rows)
    return jax.shard_map(step, mesh=mesh, in_specs=in_specs, out_specs=(spec_tok, spec_seq, spec_seq), check_vma=False)
```

```python
import functools

import jax
import jax.numpy as jnp
from jax import lax
from jax.experimental import pallas as pl
from jax.experimental.pallas import tpu as pltpu
from jax.sharding import PartitionSpec as P


F32 = jnp.float32
BF16 = jnp.bfloat16
NEG = -1e30
LOG2E = 1.4426950408889634
COL_TILE = 512
COL_CHUNKS = 2
HEADS_PER_STEP = 4
W_SLOTS = 4


def rms_norm(values, gain_vec):
    inv_rms = lax.rsqrt(jnp.mean(values * values, axis=-1, keepdims=True) + 1e-6)
    return values * inv_rms * gain_vec


def apply_rope(values, cos_tab, sin_tab):
    half_dim = values.shape[-1] // 2
    lower_half = values[..., :half_dim]
    upper_half = values[..., half_dim:]
    return jnp.concatenate([lower_half * cos_tab - upper_half * sin_tab, upper_half * cos_tab + lower_half * sin_tab], axis=-1)


def attention_kernel(scal_ref, q_ref, k_old_ref, k_new_ref, v_old_ref, v_new_ref, r_ref, cos_ref, sin_ref, o_ref, *, scale):
    heads, _, m_rows = q_ref.shape
    nope = k_old_ref.shape[2]
    prefix = k_old_ref.shape[1]
    rope_half = cos_ref.shape[0]
    blk = m_rows
    factor = scale * LOG2E
    cos_tab = cos_ref[...]
    sin_tab = sin_ref[...]
    pad_row = lax.broadcasted_iota(jnp.int32, (nope - 2 * rope_half, m_rows), 0)
    ones_row = jnp.where(pad_row == 0, 1.0, 0.0).astype(BF16)
    half = m_rows // 2
    qlane = lax.broadcasted_iota(jnp.int32, (blk, m_rows), 1)
    krow = lax.broadcasted_iota(jnp.int32, (blk, m_rows), 0)
    q_blk0 = scal_ref[0]
    q_blk1 = scal_ref[1]
    base = scal_ref[2] * m_rows
    qpos = jnp.where(qlane < half, q_blk0 * half + qlane, q_blk1 * half + qlane - half) - base
    causal = krow <= qpos

    def body(new_blocks):
        for h in range(heads):
            low = q_ref[h, nope:nope + rope_half, :]
            high = q_ref[h, nope + rope_half:, :]
            q_cat = jnp.concatenate([
                q_ref[h, :nope, :].astype(BF16),
                (low * cos_tab - high * sin_tab).astype(BF16),
                (high * cos_tab + low * sin_tab).astype(BF16),
                ones_row], axis=0)
            scores = []
            for i in range(prefix // blk + new_blocks):
                start = i * blk
                if start < prefix:
                    k_part = k_old_ref[h, start:start + blk, :]
                else:
                    k_part = k_new_ref[h, start - prefix:start - prefix + blk, :]
                k_cat = jnp.concatenate([k_part, r_ref[start:start + blk, :]], axis=1)
                s = jnp.dot(k_cat, q_cat, preferred_element_type=F32)
                if i == prefix // blk + new_blocks - 1:
                    s = jnp.where(causal, s, NEG)
                scores.append(s)
            top = functools.reduce(jnp.maximum, scores)
            top = jnp.max(top, axis=0, keepdims=True)
            total = None
            out = None
            for i, s in enumerate(scores):
                start = i * blk
                e = jnp.exp2((s - top) * factor)
                part = jnp.sum(e, axis=0, keepdims=True)
                total = part if total is None else total + part
                if start < prefix:
                    v_part = v_old_ref[h, :, start:start + blk]
                else:
                    v_part = v_new_ref[h, :, start - prefix:start - prefix + blk]
                o_part = jnp.dot(v_part, e.astype(BF16), preferred_element_type=F32)
                out = o_part if out is None else out + o_part
            out = out * (1.0 / total)
            o_ref[:, h * nope:(h + 1) * nope] = out.T.astype(BF16)

    for c in range(v_new_ref.shape[2] // blk):
        @pl.when(scal_ref[2] == c)
        def _(c=c):
            body(c + 1)


def attention(scal, q, q_tile, k_old, k_new, v_old, v_new, r_cat, cos_tab, sin_tab, scale):
    n_heads, q_dim, _ = q.shape
    m_rows = cos_tab.shape[1]
    prefix, nope = k_old.shape[1:]
    n_new = k_new.shape[1]
    hb = HEADS_PER_STEP
    flops = 2 * n_heads * m_rows * (prefix + n_new) * (256 + 128)
    head_blk = lambda *shape: pl.BlockSpec((hb,) + shape, lambda g, s: (g, 0, 0))
    whole = lambda *shape: pl.BlockSpec(shape, lambda g, s: (0, 0))
    return pl.pallas_call(
        functools.partial(attention_kernel, scale=scale),
        out_shape=jax.ShapeDtypeStruct((m_rows, n_heads * nope), BF16),
        grid_spec=pltpu.PrefetchScalarGridSpec(
            num_scalar_prefetch=1,
            grid=(n_heads // hb,),
            in_specs=[
                pl.BlockSpec((hb, q_dim, m_rows), lambda g, s: (g, 0, q_tile)),
                head_blk(prefix, nope),
                head_blk(n_new, nope),
                head_blk(nope, prefix),
                head_blk(nope, n_new),
                whole(*r_cat.shape),
                whole(*cos_tab.shape),
                whole(*sin_tab.shape),
            ],
            out_specs=pl.BlockSpec((m_rows, hb * nope), lambda g, s: (0, g)),
        ),
        compiler_params=pltpu.CompilerParams(dimension_semantics=("arbitrary",)),
        cost_estimate=pl.CostEstimate(flops=flops, bytes_accessed=30_000_000, transcendentals=n_heads * m_rows * (prefix + n_new)),
        name="attention",
    )(scal, q, k_old, k_new, v_old, v_new, r_cat, cos_tab, sin_tab)


def out_proj_kernel(*refs, n_in, first):
    o_hbm = refs[:n_in]
    w_hbm, near_ref, far_ref, o_buf, w_buf, o_sems, w_sems = refs[n_in:]
    j = pl.program_id(0)
    tiles = pl.num_programs(0)
    slots = w_buf.shape[0]
    half = o_buf.shape[1] // 2
    depth = w_buf.shape[1]

    def weights(tile, slot):
        col = pl.multiple_of((tile + first) * COL_TILE, COL_TILE)
        return pltpu.make_async_copy(w_hbm.at[:, pl.ds(col, COL_TILE)], w_buf.at[slot], w_sems.at[slot])

    @pl.when(j == 0)
    def _():
        weights(0, 0).start()
        loads = [pltpu.make_async_copy(o_hbm[i], o_buf.at[i, :, :depth], o_sems.at[i]) for i in range(n_in)]
        for load in loads:
            load.start()
        for slot in range(1, slots):
            weights(slot, slot).start()
        for load in loads:
            load.wait()

    slot = lax.rem(j, slots)
    weights(j, slot).wait()
    for i in range(n_in):
        prod = jnp.dot(o_buf[i, :, :depth], w_buf[slot], preferred_element_type=F32)
        near_ref[i * half:(i + 1) * half, :] = prod[:half]
        far_ref[i * half:(i + 1) * half, :] = prod[half:]

    @pl.when(j + slots < tiles)
    def _():
        weights(j + slots, slot).start()


def out_proj(o_list, w_out, first, count):
    m_rows, depth = o_list[0].shape
    n_in = len(o_list)
    half = m_rows // 2
    tiles = count // COL_TILE
    out = jax.ShapeDtypeStruct((n_in * half, count), F32)
    raw = pl.BlockSpec(memory_space=pl.ANY)
    out_spec = pl.BlockSpec((n_in * half, COL_TILE), lambda j: (0, j))
    return pl.pallas_call(
        functools.partial(out_proj_kernel, n_in=n_in, first=first // COL_TILE),
        out_shape=(out, out),
        grid=(tiles,),
        in_specs=[raw] * (n_in + 1),
        out_specs=(out_spec, out_spec),
        scratch_shapes=[
            pltpu.VMEM((n_in, m_rows, depth + 128), BF16),
            pltpu.VMEM((W_SLOTS, depth, COL_TILE), BF16),
            pltpu.SemaphoreType.DMA((n_in,)),
            pltpu.SemaphoreType.DMA((W_SLOTS,)),
        ],
        compiler_params=pltpu.CompilerParams(dimension_semantics=("arbitrary",)),
        cost_estimate=pl.CostEstimate(flops=2 * n_in * m_rows * depth * count, bytes_accessed=depth * count * 2 + n_in * m_rows * count * 4, transcendentals=0),
        name="out_proj",
    )(*o_list, w_out)


def cache_kernel(len_ref, lat_ref, lat_new_ref, pe_ref, pe_new_ref, lat_out_ref, pe_out_ref):
    start = len_ref[pl.program_id(0)]
    for old_ref, new_ref, out_ref, axis in ((lat_ref, lat_new_ref, lat_out_ref, 0), (pe_ref, pe_new_ref, pe_out_ref, 1)):
        new = new_ref[0].astype(F32)
        count = new.shape[axis]
        wide = jnp.concatenate([new, jnp.zeros_like(new)], axis=axis)
        moved = pltpu.roll(wide, start, axis)
        pos = lax.broadcasted_iota(jnp.int32, wide.shape, axis)
        inside = jnp.logical_and(pos >= start, pos < start + count)
        out_ref[0] = jnp.where(inside, moved, old_ref[0].astype(F32)).astype(BF16)


def write_caches(lengths, lat, lat_new, pe_t, pe_new_t):
    spec = lambda arr: pl.BlockSpec((1,) + arr.shape[1:], lambda b, s: (b, 0, 0))
    return pl.pallas_call(
        cache_kernel,
        out_shape=(jax.ShapeDtypeStruct(lat.shape, lat.dtype), jax.ShapeDtypeStruct(pe_t.shape, pe_t.dtype)),
        grid_spec=pltpu.PrefetchScalarGridSpec(
            num_scalar_prefetch=1,
            grid=(lat.shape[0],),
            in_specs=[spec(lat), spec(lat_new), spec(pe_t), spec(pe_new_t)],
            out_specs=(spec(lat), spec(pe_t)),
        ),
        compiler_params=pltpu.CompilerParams(dimension_semantics=("arbitrary",)),
        cost_estimate=pl.CostEstimate(flops=20_000_000, bytes_accessed=2 * lat.size * 2, transcendentals=0),
        name="write_caches",
    )(lengths, lat, lat_new, pe_t, pe_new_t)


def solution(mesh):
    tp = mesh.shape["tp"]
    to_partner = [(i, i ^ 1) for i in range(tp)]
    to_chip = [(i, i ^ 2) for i in range(tp)]

    def partner(value):
        return lax.ppermute(value, "tp", to_partner)

    def other_chip(value):
        return lax.ppermute(value, "tp", to_chip)

    def step(hidden, lengths, rope_cos, rope_sin, cache_lat, cache_pe, norm_in, w_dq, norm_q, w_dkv, norm_kv, w_uq, w_uk, w_uv, w_out):
        me = lax.axis_index("tp")
        n_seq, n_tok, model_dim = hidden.shape
        kv_rank, _, nope = w_uk.shape
        rope_dim = cache_pe.shape[2]
        n_new = rope_cos.shape[1]
        prefix = cache_lat.shape[1] - n_new
        q_rank = w_dq.shape[1]
        scale = (nope + rope_dim) ** -0.5

        normed = rms_norm(hidden.astype(F32), norm_in).astype(BF16).reshape(n_seq * n_tok, model_dim)
        kv_proj = jnp.dot(normed, w_dkv, preferred_element_type=F32).reshape(n_seq, n_tok, kv_rank + rope_dim)
        my_cos = lax.dynamic_slice_in_dim(rope_cos, me * n_tok, n_tok, axis=1)
        my_sin = lax.dynamic_slice_in_dim(rope_sin, me * n_tok, n_tok, axis=1)
        my_lat = rms_norm(kv_proj[..., :kv_rank], norm_kv).astype(BF16)
        my_pe = apply_rope(kv_proj[..., kv_rank:], my_cos, my_sin).astype(BF16)
        my_kv = jnp.concatenate([my_lat, my_pe], axis=-1)
        my_q = rms_norm(jnp.dot(normed, w_dq, preferred_element_type=F32), norm_q).astype(BF16).reshape(n_seq, n_tok, q_rank)

        def gather(value):
            far = other_chip(value)
            near = partner(value)
            return [value, near, far, partner(far)]

        kv_rel = jnp.stack(gather(my_kv))
        kv_true = jnp.concatenate([lax.dynamic_index_in_dim(kv_rel, me ^ j, keepdims=False) for j in range(tp)], axis=1)
        lat_new = kv_true[..., :kv_rank]
        pe_new = kv_true[..., kv_rank:]
        q_rel = [gather(my_q[b]) for b in range(n_seq)]

        def project(lat):
            keys = jnp.einsum("sc,chd->hsd", lat, w_uk, preferred_element_type=F32).astype(BF16)
            values = jnp.einsum("chv,sc->hvs", w_uv, lat, preferred_element_type=F32).astype(BF16)
            return keys, values

        row = jnp.arange(prefix)
        alive = row[None, :] < lengths[:, None]
        old_lat = jnp.where(alive[..., None], cache_lat[:, :prefix], 0)
        old_pe = jnp.where(alive[..., None], cache_pe[:, :prefix], 0)
        kv_old = [project(old_lat[b]) for b in range(n_seq)]
        kv_new = [project(lat_new[b]) for b in range(n_seq)]
        bias = jnp.where(alive, 0.0, NEG).astype(BF16)[..., None]
        pad_old = jnp.zeros((n_seq, prefix, nope - rope_dim - 1), BF16)
        pad_new = jnp.zeros((n_seq, n_new, nope - rope_dim), BF16)
        r_cat = jnp.concatenate([
            jnp.concatenate([old_pe, bias, pad_old], axis=-1),
            jnp.concatenate([pe_new, pad_new], axis=-1)], axis=1)

        def queries(q_lat):
            return jnp.einsum("qhd,tq->hdt", w_uq, q_lat, preferred_element_type=F32)

        def attend(rel, b, q, q_tile):
            blocks = (me ^ rel, me ^ (rel + 1))
            scal = jnp.stack([blocks[0], blocks[1], blocks[0] // 2]).astype(jnp.int32)
            cut = lambda tab: jnp.concatenate([lax.dynamic_slice_in_dim(tab[b], k * n_tok, n_tok, axis=0) for k in blocks], axis=0).T
            return attention(scal, q, q_tile, kv_old[b][0], kv_new[b][0], kv_old[b][1], kv_new[b][1], r_cat[b], cut(rope_cos), cut(rope_sin), scale)

        def after(value, *deps):
            return lax.optimization_barrier((value,) + deps)[0]

        width = model_dim // COL_CHUNKS
        arrived = [[None] * COL_CHUNKS for _ in range(n_seq)]
        pending = []

        def send_one():
            b, j, near_part, came = pending.pop(0)
            summed = near_part + came
            arrived[b][j] = other_chip(summed)
            return summed

        near_part = None
        for b in range(n_seq):
            q_lat = jnp.concatenate(q_rel[b][2:], axis=0)
            if near_part is not None:
                q_lat = after(q_lat, near_part)
            q = queries(q_lat)
            if pending:
                q = after(q, send_one())
            o = attend(2, b, q, 0)
            for j in range(COL_CHUNKS):
                if len(pending) > 1 - (j == 0):
                    o = after(o, send_one())
                near_part, far_part = out_proj([o], w_out, j * width, width)
                pending.append((b, j, near_part, partner(far_part)))
        q_lat = jnp.concatenate([q_rel[b][k] for b in range(n_seq) for k in (0, 1)], axis=0)
        q_own = queries(after(q_lat, near_part))
        dep = (send_one(),)
        o_own = []
        for b in range(n_seq):
            o_own.append(attend(0, b, after(q_own, *dep), b))
            dep = (o_own[-1],) + ((send_one(),) if pending else ())
        cols = []
        flat = hidden.reshape(n_seq * n_tok, model_dim)
        for j in range(COL_CHUNKS):
            own_part, partner_part = out_proj([after(o_own[0], *dep), o_own[1]], w_out, j * width, width)
            dep = (own_part,)
            base = own_part + partner(partner_part) + flat[:, j * width:(j + 1) * width].astype(F32)
            cols.append(base + jnp.concatenate([arrived[b][j] for b in range(n_seq)], axis=0))
        out = jnp.concatenate(cols, axis=1).astype(BF16).reshape(hidden.shape)
        lat_all, pe_all_t = write_caches(lengths, cache_lat, lat_new, cache_pe.transpose(0, 2, 1), pe_new.transpose(0, 2, 1))
        pe_all = pe_all_t.transpose(0, 2, 1)
        return out, lat_all, pe_all

    spec_tok = P("dp", "tp", None)
    spec_len = P("dp")
    spec_seq = P("dp", None, None)
    spec_vec = P(None)
    spec_mat = P(None, None)
    spec_head = P(None, "tp", None)
    spec_rows = P("tp", None)
    in_specs = (spec_tok, spec_len, spec_seq, spec_seq, spec_seq, spec_seq, spec_vec, spec_mat, spec_vec, spec_mat, spec_vec, spec_head, spec_head, spec_head, spec_rows)
    return jax.shard_map(step, mesh=mesh, in_specs=in_specs, out_specs=(spec_tok, spec_seq, spec_seq), check_vma=False)
```

```python
import functools

import jax
import jax.numpy as jnp
from jax import lax
from jax.experimental import pallas as pl
from jax.experimental.pallas import tpu as pltpu
from jax.sharding import PartitionSpec as P


F32 = jnp.float32
BF16 = jnp.bfloat16
NEG = -1e30
LOG2E = 1.4426950408889634
COL_TILE = 512
FAR_WIDTHS = (1536, 2560, 3072)
OWN_WIDTHS = (4096, 3072)
HEADS_PER_STEP = 4
W_SLOTS = 4


def rms_norm(values, gain_vec):
    inv_rms = lax.rsqrt(jnp.mean(values * values, axis=-1, keepdims=True) + 1e-6)
    return values * inv_rms * gain_vec


def apply_rope(values, cos_tab, sin_tab):
    half_dim = values.shape[-1] // 2
    lower_half = values[..., :half_dim]
    upper_half = values[..., half_dim:]
    return jnp.concatenate([lower_half * cos_tab - upper_half * sin_tab, upper_half * cos_tab + lower_half * sin_tab], axis=-1)


def attention_kernel(scal_ref, q_ref, k_old_ref, k_new_ref, v_old_ref, v_new_ref, r_ref, cos_ref, sin_ref, o_ref, *, scale):
    heads, _, m_rows = q_ref.shape
    nope = k_old_ref.shape[2]
    prefix = k_old_ref.shape[1]
    rope_half = cos_ref.shape[0]
    blk = m_rows
    factor = scale * LOG2E
    cos_tab = cos_ref[...]
    sin_tab = sin_ref[...]
    pad_row = lax.broadcasted_iota(jnp.int32, (nope - 2 * rope_half, m_rows), 0)
    ones_row = jnp.where(pad_row == 0, 1.0, 0.0).astype(BF16)
    half = m_rows // 2
    qlane = lax.broadcasted_iota(jnp.int32, (blk, m_rows), 1)
    krow = lax.broadcasted_iota(jnp.int32, (blk, m_rows), 0)
    q_blk0 = scal_ref[0]
    q_blk1 = scal_ref[1]
    base = scal_ref[2] * m_rows
    qpos = jnp.where(qlane < half, q_blk0 * half + qlane, q_blk1 * half + qlane - half) - base
    causal = krow <= qpos

    def body(new_blocks):
        for h in range(heads):
            low = q_ref[h, nope:nope + rope_half, :]
            high = q_ref[h, nope + rope_half:, :]
            q_cat = jnp.concatenate([
                q_ref[h, :nope, :].astype(BF16),
                (low * cos_tab - high * sin_tab).astype(BF16),
                (high * cos_tab + low * sin_tab).astype(BF16),
                ones_row], axis=0)
            scores = []
            for i in range(prefix // blk + new_blocks):
                start = i * blk
                if start < prefix:
                    k_part = k_old_ref[h, start:start + blk, :]
                else:
                    k_part = k_new_ref[h, start - prefix:start - prefix + blk, :]
                k_cat = jnp.concatenate([k_part, r_ref[start:start + blk, :]], axis=1)
                s = jnp.dot(k_cat, q_cat, preferred_element_type=F32)
                if i == prefix // blk + new_blocks - 1:
                    s = jnp.where(causal, s, NEG)
                scores.append(s)
            top = functools.reduce(jnp.maximum, scores)
            top = jnp.max(top, axis=0, keepdims=True)
            total = None
            out = None
            for i, s in enumerate(scores):
                start = i * blk
                e = jnp.exp2((s - top) * factor)
                part = jnp.sum(e, axis=0, keepdims=True)
                total = part if total is None else total + part
                if start < prefix:
                    v_part = v_old_ref[h, :, start:start + blk]
                else:
                    v_part = v_new_ref[h, :, start - prefix:start - prefix + blk]
                o_part = jnp.dot(v_part, e.astype(BF16), preferred_element_type=F32)
                out = o_part if out is None else out + o_part
            out = out * (1.0 / total)
            o_ref[:, h * nope:(h + 1) * nope] = out.T.astype(BF16)

    for c in range(v_new_ref.shape[2] // blk):
        @pl.when(scal_ref[2] == c)
        def _(c=c):
            body(c + 1)


def attention(scal, q, q_tile, k_old, k_new, v_old, v_new, r_cat, cos_tab, sin_tab, scale):
    n_heads, q_dim, _ = q.shape
    m_rows = cos_tab.shape[1]
    prefix, nope = k_old.shape[1:]
    n_new = k_new.shape[1]
    hb = HEADS_PER_STEP
    flops = 2 * n_heads * m_rows * (prefix + n_new) * (256 + 128)
    head_blk = lambda *shape: pl.BlockSpec((hb,) + shape, lambda g, s: (g, 0, 0))
    whole = lambda *shape: pl.BlockSpec(shape, lambda g, s: (0, 0))
    return pl.pallas_call(
        functools.partial(attention_kernel, scale=scale),
        out_shape=jax.ShapeDtypeStruct((m_rows, n_heads * nope), BF16),
        grid_spec=pltpu.PrefetchScalarGridSpec(
            num_scalar_prefetch=1,
            grid=(n_heads // hb,),
            in_specs=[
                pl.BlockSpec((hb, q_dim, m_rows), lambda g, s: (g, 0, q_tile)),
                head_blk(prefix, nope),
                head_blk(n_new, nope),
                head_blk(nope, prefix),
                head_blk(nope, n_new),
                whole(*r_cat.shape),
                whole(*cos_tab.shape),
                whole(*sin_tab.shape),
            ],
            out_specs=pl.BlockSpec((m_rows, hb * nope), lambda g, s: (0, g)),
        ),
        compiler_params=pltpu.CompilerParams(dimension_semantics=("arbitrary",)),
        cost_estimate=pl.CostEstimate(flops=flops, bytes_accessed=30_000_000, transcendentals=n_heads * m_rows * (prefix + n_new)),
        name="attention",
    )(scal, q, k_old, k_new, v_old, v_new, r_cat, cos_tab, sin_tab)


def out_proj_kernel(*refs, n_in, first):
    o_hbm = refs[:n_in]
    w_hbm, near_ref, far_ref, o_buf, w_buf, o_sems, w_sems = refs[n_in:]
    j = pl.program_id(0)
    tiles = pl.num_programs(0)
    slots = w_buf.shape[0]
    m_rows = o_buf.shape[0] // n_in
    half = m_rows // 2

    def weights(tile, slot):
        col = pl.multiple_of((tile + first) * COL_TILE, COL_TILE)
        return pltpu.make_async_copy(w_hbm.at[:, pl.ds(col, COL_TILE)], w_buf.at[slot], w_sems.at[slot])

    @pl.when(j == 0)
    def _():
        weights(0, 0).start()
        loads = [pltpu.make_async_copy(o_hbm[i], o_buf.at[pl.ds(i * m_rows, m_rows)], o_sems.at[i]) for i in range(n_in)]
        for load in loads:
            load.start()
        for slot in range(1, slots):
            weights(slot, slot).start()
        for load in loads:
            load.wait()

    slot = lax.rem(j, slots)
    weights(j, slot).wait()
    prod = jnp.dot(o_buf[:, :], w_buf[slot], preferred_element_type=F32)
    for i in range(n_in):
        near_ref[i * half:(i + 1) * half, :] = prod[2 * i * half:(2 * i + 1) * half]
        far_ref[i * half:(i + 1) * half, :] = prod[(2 * i + 1) * half:(2 * i + 2) * half]

    @pl.when(j + slots < tiles)
    def _():
        weights(j + slots, slot).start()


def out_proj(o_list, w_out, first, count):
    m_rows, depth = o_list[0].shape
    n_in = len(o_list)
    half = m_rows // 2
    tiles = count // COL_TILE
    slots = min(W_SLOTS, tiles)
    out = jax.ShapeDtypeStruct((n_in * half, count), F32)
    raw = pl.BlockSpec(memory_space=pl.ANY)
    out_spec = pl.BlockSpec((n_in * half, COL_TILE), lambda j: (0, j))
    return pl.pallas_call(
        functools.partial(out_proj_kernel, n_in=n_in, first=first // COL_TILE),
        out_shape=(out, out),
        grid=(tiles,),
        in_specs=[raw] * (n_in + 1),
        out_specs=(out_spec, out_spec),
        scratch_shapes=[
            pltpu.VMEM((n_in * m_rows, depth), BF16),
            pltpu.VMEM((slots, depth, COL_TILE), BF16),
            pltpu.SemaphoreType.DMA((n_in,)),
            pltpu.SemaphoreType.DMA((slots,)),
        ],
        compiler_params=pltpu.CompilerParams(dimension_semantics=("arbitrary",)),
        cost_estimate=pl.CostEstimate(flops=2 * n_in * m_rows * depth * count, bytes_accessed=depth * count * 2 + n_in * m_rows * count * 4, transcendentals=0),
        name="out_proj",
    )(*o_list, w_out)


def cache_kernel(len_ref, lat_ref, lat_new_ref, pe_ref, pe_new_ref, lat_out_ref, pe_out_ref):
    start = len_ref[pl.program_id(0)]
    for old_ref, new_ref, out_ref, axis in ((lat_ref, lat_new_ref, lat_out_ref, 0), (pe_ref, pe_new_ref, pe_out_ref, 1)):
        new = new_ref[0].astype(F32)
        count = new.shape[axis]
        wide = jnp.concatenate([new, jnp.zeros_like(new)], axis=axis)
        moved = pltpu.roll(wide, start, axis)
        pos = lax.broadcasted_iota(jnp.int32, wide.shape, axis)
        inside = jnp.logical_and(pos >= start, pos < start + count)
        out_ref[0] = jnp.where(inside, moved, old_ref[0].astype(F32)).astype(BF16)


def write_caches(lengths, lat, lat_new, pe_t, pe_new_t):
    spec = lambda arr: pl.BlockSpec((1,) + arr.shape[1:], lambda b, s: (b, 0, 0))
    return pl.pallas_call(
        cache_kernel,
        out_shape=(jax.ShapeDtypeStruct(lat.shape, lat.dtype), jax.ShapeDtypeStruct(pe_t.shape, pe_t.dtype)),
        grid_spec=pltpu.PrefetchScalarGridSpec(
            num_scalar_prefetch=1,
            grid=(lat.shape[0],),
            in_specs=[spec(lat), spec(lat_new), spec(pe_t), spec(pe_new_t)],
            out_specs=(spec(lat), spec(pe_t)),
        ),
        compiler_params=pltpu.CompilerParams(dimension_semantics=("arbitrary",)),
        cost_estimate=pl.CostEstimate(flops=20_000_000, bytes_accessed=2 * lat.size * 2, transcendentals=0),
        name="write_caches",
    )(lengths, lat, lat_new, pe_t, pe_new_t)


def solution(mesh):
    tp = mesh.shape["tp"]
    to_partner = [(i, i ^ 1) for i in range(tp)]
    to_chip = [(i, i ^ 2) for i in range(tp)]

    def partner(value):
        return lax.ppermute(value, "tp", to_partner)

    def other_chip(value):
        return lax.ppermute(value, "tp", to_chip)

    def step(hidden, lengths, rope_cos, rope_sin, cache_lat, cache_pe, norm_in, w_dq, norm_q, w_dkv, norm_kv, w_uq, w_uk, w_uv, w_out):
        me = lax.axis_index("tp")
        n_seq, n_tok, model_dim = hidden.shape
        kv_rank, _, nope = w_uk.shape
        rope_dim = cache_pe.shape[2]
        n_new = rope_cos.shape[1]
        prefix = cache_lat.shape[1] - n_new
        q_rank = w_dq.shape[1]
        scale = (nope + rope_dim) ** -0.5

        normed = rms_norm(hidden.astype(F32), norm_in).astype(BF16).reshape(n_seq * n_tok, model_dim)
        kv_proj = jnp.dot(normed, w_dkv, preferred_element_type=F32).reshape(n_seq, n_tok, kv_rank + rope_dim)
        my_cos = lax.dynamic_slice_in_dim(rope_cos, me * n_tok, n_tok, axis=1)
        my_sin = lax.dynamic_slice_in_dim(rope_sin, me * n_tok, n_tok, axis=1)
        my_lat = rms_norm(kv_proj[..., :kv_rank], norm_kv).astype(BF16)
        my_pe = apply_rope(kv_proj[..., kv_rank:], my_cos, my_sin).astype(BF16)
        my_kv = jnp.concatenate([my_lat, my_pe], axis=-1)
        my_q = rms_norm(jnp.dot(normed, w_dq, preferred_element_type=F32), norm_q).astype(BF16).reshape(n_seq, n_tok, q_rank)

        def gather(value):
            far = other_chip(value)
            near = partner(value)
            return [value, near, far, partner(far)]

        kv_rel = jnp.stack(gather(my_kv))
        kv_true = jnp.concatenate([lax.dynamic_index_in_dim(kv_rel, me ^ j, keepdims=False) for j in range(tp)], axis=1)
        lat_new = kv_true[..., :kv_rank]
        pe_new = kv_true[..., kv_rank:]
        q_rel = [gather(my_q[b]) for b in range(n_seq)]

        def project(lat):
            keys = jnp.einsum("sc,chd->hsd", lat, w_uk, preferred_element_type=F32).astype(BF16)
            values = jnp.einsum("chv,sc->hvs", w_uv, lat, preferred_element_type=F32).astype(BF16)
            return keys, values

        row = jnp.arange(prefix)
        alive = row[None, :] < lengths[:, None]
        old_lat = jnp.where(alive[..., None], cache_lat[:, :prefix], 0)
        old_pe = jnp.where(alive[..., None], cache_pe[:, :prefix], 0)
        kv_old = [project(old_lat[b]) for b in range(n_seq)]
        kv_new = [project(lat_new[b]) for b in range(n_seq)]
        bias = jnp.where(alive, 0.0, NEG).astype(BF16)[..., None]
        pad_old = jnp.zeros((n_seq, prefix, nope - rope_dim - 1), BF16)
        pad_new = jnp.zeros((n_seq, n_new, nope - rope_dim), BF16)
        r_cat = jnp.concatenate([
            jnp.concatenate([old_pe, bias, pad_old], axis=-1),
            jnp.concatenate([pe_new, pad_new], axis=-1)], axis=1)

        def queries(q_lat):
            return jnp.einsum("qhd,tq->hdt", w_uq, q_lat, preferred_element_type=F32)

        def attend(rel, b, q, q_tile):
            blocks = (me ^ rel, me ^ (rel + 1))
            scal = jnp.stack([blocks[0], blocks[1], blocks[0] // 2]).astype(jnp.int32)
            cut = lambda tab: jnp.concatenate([lax.dynamic_slice_in_dim(tab[b], k * n_tok, n_tok, axis=0) for k in blocks], axis=0).T
            return attention(scal, q, q_tile, kv_old[b][0], kv_new[b][0], kv_old[b][1], kv_new[b][1], r_cat[b], cut(rope_cos), cut(rope_sin), scale)

        def after(value, *deps):
            return lax.optimization_barrier((value,) + deps)[0]

        def tokens(rel):
            return jnp.concatenate([q_rel[b][k] for b in range(n_seq) for k in (rel, rel + 1)], axis=0)

        arrived = []
        pending = []

        def send_one():
            near_part, came = pending.pop(0)
            summed = near_part + came
            arrived.append(other_chip(summed))
            return summed

        q_far = queries(tokens(2))
        o_far = []
        for b in range(n_seq):
            o_far.append(attend(2, b, after(q_far, *o_far), b))
        first = 0
        for j, width in enumerate(FAR_WIDTHS):
            deps = (send_one(),) if len(pending) > 1 else ()
            if j:
                deps += (near_part,)
            near_part, far_part = out_proj([after(o_far[0], *deps), o_far[1]], w_out, first, width)
            pending.append((near_part, partner(far_part)))
            first += width
        q_own = queries(after(tokens(0), near_part))
        dep = (send_one(),)
        o_own = []
        for b in range(n_seq):
            o_own.append(attend(0, b, after(q_own, *dep), b))
            dep = (o_own[-1],) + ((send_one(),) if pending else ())
        flat = hidden.reshape(n_seq * n_tok, model_dim)
        base = []
        first = 0
        for width in OWN_WIDTHS:
            own_part, partner_part = out_proj([after(o_own[0], *dep), o_own[1]], w_out, first, width)
            dep = (own_part,)
            base.append(own_part + partner(partner_part))
            first += width
        total = jnp.concatenate(base, axis=1) + flat.astype(F32) + jnp.concatenate(arrived, axis=1)
        out = total.astype(BF16).reshape(hidden.shape)
        lat_all, pe_all_t = write_caches(lengths, cache_lat, lat_new, cache_pe.transpose(0, 2, 1), pe_new.transpose(0, 2, 1))
        pe_all = pe_all_t.transpose(0, 2, 1)
        return out, lat_all, pe_all

    spec_tok = P("dp", "tp", None)
    spec_len = P("dp")
    spec_seq = P("dp", None, None)
    spec_vec = P(None)
    spec_mat = P(None, None)
    spec_head = P(None, "tp", None)
    spec_rows = P("tp", None)
    in_specs = (spec_tok, spec_len, spec_seq, spec_seq, spec_seq, spec_seq, spec_vec, spec_mat, spec_vec, spec_mat, spec_vec, spec_head, spec_head, spec_head, spec_rows)
    return jax.shard_map(step, mesh=mesh, in_specs=in_specs, out_specs=(spec_tok, spec_seq, spec_seq), check_vma=False)
```

```python
import functools

import jax
import jax.numpy as jnp
from jax import lax
from jax.experimental import pallas as pl
from jax.experimental.pallas import tpu as pltpu
from jax.sharding import PartitionSpec as P


F32 = jnp.float32
BF16 = jnp.bfloat16
NEG = -1e30
LOG2E = 1.4426950408889634
COL_TILE = 512
FAR_WIDTHS = (1536, 2048, 3584)
OWN_WIDTHS = (4096, 3072)
HEADS_PER_STEP = 8
HEADS_UNROLLED = 2
W_SLOTS = 4


def rms_norm(values, gain_vec):
    inv_rms = lax.rsqrt(jnp.mean(values * values, axis=-1, keepdims=True) + 1e-6)
    return values * inv_rms * gain_vec


def apply_rope(values, cos_tab, sin_tab):
    half_dim = values.shape[-1] // 2
    lower_half = values[..., :half_dim]
    upper_half = values[..., half_dim:]
    return jnp.concatenate([lower_half * cos_tab - upper_half * sin_tab, upper_half * cos_tab + lower_half * sin_tab], axis=-1)


def latent_kernel(lat_ref, wk_ref, wv_ref, k_ref, v_ref, wk_buf, wv_buf):
    n_seq, heads, _, dim = k_ref.shape
    wk_buf[...] = jnp.swapaxes(wk_ref[...].astype(F32), 0, 1).astype(BF16)
    wv_buf[...] = jnp.swapaxes(wv_ref[...].astype(F32), 0, 1).astype(BF16)

    @pl.loop(0, heads // 2)
    def _(pair):
        h = pair * 2
        wk = jnp.concatenate([wk_buf[h], wk_buf[h + 1]], axis=1)
        wv = jnp.concatenate([wv_buf[h], wv_buf[h + 1]], axis=1)
        for b in range(n_seq):
            lat = lat_ref[b]
            keys = jnp.dot(lat, wk, preferred_element_type=F32)
            values = jnp.dot(lat, wv, preferred_element_type=F32)
            for i in range(2):
                k_ref[b, h + i] = keys[:, i * dim:(i + 1) * dim].astype(BF16)
                v_ref[b, h + i] = values[:, i * dim:(i + 1) * dim].T.astype(BF16)


def latent_project(lat, w_uk, w_uv):
    n_seq, n_rows, rank = lat.shape
    _, n_heads, dim = w_uk.shape
    group = 8
    w_spec = pl.BlockSpec((rank, group, dim), lambda g: (0, g, 0))
    return pl.pallas_call(
        latent_kernel,
        out_shape=(
            jax.ShapeDtypeStruct((n_seq, n_heads, n_rows, dim), BF16),
            jax.ShapeDtypeStruct((n_seq, n_heads, dim, n_rows), BF16),
        ),
        grid=(n_heads // group,),
        in_specs=[pl.BlockSpec(lat.shape, lambda g: (0, 0, 0)), w_spec, w_spec],
        out_specs=(
            pl.BlockSpec((n_seq, group, n_rows, dim), lambda g: (0, g, 0, 0)),
            pl.BlockSpec((n_seq, group, dim, n_rows), lambda g: (0, g, 0, 0)),
        ),
        scratch_shapes=[pltpu.VMEM((group, rank, dim), BF16), pltpu.VMEM((group, rank, dim), BF16)],
        compiler_params=pltpu.CompilerParams(dimension_semantics=("arbitrary",)),
        cost_estimate=pl.CostEstimate(flops=4 * n_seq * n_rows * rank * n_heads * dim, bytes_accessed=25_000_000, transcendentals=0),
        name="latent_project",
    )(lat, w_uk, w_uv)


def attention_kernel(scal_ref, q_ref, k_old_ref, k_new_ref, v_old_ref, v_new_ref, r_ref, cos_ref, sin_ref, o_ref, *, scale):
    heads, _, m_rows = q_ref.shape
    nope = k_old_ref.shape[2]
    prefix = k_old_ref.shape[1]
    rope_half = cos_ref.shape[0]
    blk = m_rows
    factor = scale * LOG2E
    cos_tab = cos_ref[...]
    sin_tab = sin_ref[...]
    pad_row = lax.broadcasted_iota(jnp.int32, (nope - 2 * rope_half, m_rows), 0)
    ones_row = jnp.where(pad_row == 0, 1.0, 0.0).astype(BF16)
    half = m_rows // 2
    qlane = lax.broadcasted_iota(jnp.int32, (blk, m_rows), 1)
    krow = lax.broadcasted_iota(jnp.int32, (blk, m_rows), 0)
    q_blk0 = scal_ref[0]
    q_blk1 = scal_ref[1]
    base = scal_ref[2] * m_rows
    qpos = jnp.where(qlane < half, q_blk0 * half + qlane, q_blk1 * half + qlane - half) - base
    causal = krow <= qpos

    def one_head(h, new_blocks):
        low = q_ref[h, nope:nope + rope_half, :]
        high = q_ref[h, nope + rope_half:, :]
        q_cat = jnp.concatenate([
            q_ref[h, :nope, :].astype(BF16),
            (low * cos_tab - high * sin_tab).astype(BF16),
            (high * cos_tab + low * sin_tab).astype(BF16),
            ones_row], axis=0)
        scores = []
        for i in range(prefix // blk + new_blocks):
            start = i * blk
            if start < prefix:
                k_part = k_old_ref[h, start:start + blk, :]
            else:
                k_part = k_new_ref[h, start - prefix:start - prefix + blk, :]
            k_cat = jnp.concatenate([k_part, r_ref[start:start + blk, :]], axis=1)
            s = jnp.dot(k_cat, q_cat, preferred_element_type=F32)
            if i == prefix // blk + new_blocks - 1:
                s = jnp.where(causal, s, NEG)
            scores.append(s)
        top = functools.reduce(jnp.maximum, scores)
        top = jnp.max(top, axis=0, keepdims=True)
        total = None
        out = None
        for i, s in enumerate(scores):
            start = i * blk
            e = jnp.exp2((s - top) * factor)
            part = jnp.sum(e, axis=0, keepdims=True)
            total = part if total is None else total + part
            if start < prefix:
                v_part = v_old_ref[h, :, start:start + blk]
            else:
                v_part = v_new_ref[h, :, start - prefix:start - prefix + blk]
            o_part = jnp.dot(v_part, e.astype(BF16), preferred_element_type=F32)
            out = o_part if out is None else out + o_part
        out = out * (1.0 / total)
        o_ref[:, pl.ds(pl.multiple_of(h * nope, nope), nope)] = out.T.astype(BF16)

    def body(new_blocks):
        @pl.loop(0, heads // HEADS_UNROLLED)
        def _(g):
            for i in range(HEADS_UNROLLED):
                one_head(g * HEADS_UNROLLED + i, new_blocks)

    for c in range(v_new_ref.shape[2] // blk):
        @pl.when(scal_ref[2] == c)
        def _(c=c):
            body(c + 1)


def attention(scal, q, q_tile, seq, k_old, k_new, v_old, v_new, r_cat, cos_tab, sin_tab, scale):
    n_heads, q_dim, _ = q.shape
    m_rows = cos_tab.shape[1]
    prefix, nope = k_old.shape[2:]
    n_new = k_new.shape[2]
    hb = HEADS_PER_STEP
    flops = 2 * n_heads * m_rows * (prefix + n_new) * (256 + 128)
    head_blk = lambda *shape: pl.BlockSpec((None, hb) + shape, lambda g, s: (seq, g, 0, 0))
    whole = lambda *shape: pl.BlockSpec(shape, lambda g, s: (0, 0))
    return pl.pallas_call(
        functools.partial(attention_kernel, scale=scale),
        out_shape=jax.ShapeDtypeStruct((m_rows, n_heads * nope), BF16),
        grid_spec=pltpu.PrefetchScalarGridSpec(
            num_scalar_prefetch=1,
            grid=(n_heads // hb,),
            in_specs=[
                pl.BlockSpec((hb, q_dim, m_rows), lambda g, s: (g, 0, q_tile)),
                head_blk(prefix, nope),
                head_blk(n_new, nope),
                head_blk(nope, prefix),
                head_blk(nope, n_new),
                whole(*r_cat.shape),
                whole(*cos_tab.shape),
                whole(*sin_tab.shape),
            ],
            out_specs=pl.BlockSpec((m_rows, hb * nope), lambda g, s: (0, g)),
        ),
        compiler_params=pltpu.CompilerParams(dimension_semantics=("arbitrary",)),
        cost_estimate=pl.CostEstimate(flops=flops, bytes_accessed=30_000_000, transcendentals=n_heads * m_rows * (prefix + n_new)),
        name="attention",
    )(scal, q, k_old, k_new, v_old, v_new, r_cat, cos_tab, sin_tab)


def out_proj_kernel(*refs, n_in, first):
    o_hbm = refs[:n_in]
    w_hbm, near_ref, far_ref, o_buf, w_buf, o_sems, w_sems = refs[n_in:]
    j = pl.program_id(0)
    tiles = pl.num_programs(0)
    slots = w_buf.shape[0]
    m_rows = o_buf.shape[0] // n_in
    half = m_rows // 2

    def weights(tile, slot):
        col = pl.multiple_of((tile + first) * COL_TILE, COL_TILE)
        return pltpu.make_async_copy(w_hbm.at[:, pl.ds(col, COL_TILE)], w_buf.at[slot], w_sems.at[slot])

    @pl.when(j == 0)
    def _():
        weights(0, 0).start()
        loads = [pltpu.make_async_copy(o_hbm[i], o_buf.at[pl.ds(i * m_rows, m_rows)], o_sems.at[i]) for i in range(n_in)]
        for load in loads:
            load.start()
        for slot in range(1, slots):
            weights(slot, slot).start()
        for load in loads:
            load.wait()

    slot = lax.rem(j, slots)
    weights(j, slot).wait()
    prod = jnp.dot(o_buf[:, :], w_buf[slot], preferred_element_type=F32)
    for i in range(n_in):
        near_ref[i * half:(i + 1) * half, :] = prod[2 * i * half:(2 * i + 1) * half]
        far_ref[i * half:(i + 1) * half, :] = prod[(2 * i + 1) * half:(2 * i + 2) * half]

    @pl.when(j + slots < tiles)
    def _():
        weights(j + slots, slot).start()


def out_proj(o_list, w_out, first, count):
    m_rows, depth = o_list[0].shape
    n_in = len(o_list)
    half = m_rows // 2
    tiles = count // COL_TILE
    slots = min(W_SLOTS, tiles)
    out = jax.ShapeDtypeStruct((n_in * half, count), F32)
    raw = pl.BlockSpec(memory_space=pl.ANY)
    out_spec = pl.BlockSpec((n_in * half, COL_TILE), lambda j: (0, j))
    return pl.pallas_call(
        functools.partial(out_proj_kernel, n_in=n_in, first=first // COL_TILE),
        out_shape=(out, out),
        grid=(tiles,),
        in_specs=[raw] * (n_in + 1),
        out_specs=(out_spec, out_spec),
        scratch_shapes=[
            pltpu.VMEM((n_in * m_rows, depth), BF16),
            pltpu.VMEM((slots, depth, COL_TILE), BF16),
            pltpu.SemaphoreType.DMA((n_in,)),
            pltpu.SemaphoreType.DMA((slots,)),
        ],
        compiler_params=pltpu.CompilerParams(dimension_semantics=("arbitrary",)),
        cost_estimate=pl.CostEstimate(flops=2 * n_in * m_rows * depth * count, bytes_accessed=depth * count * 2 + n_in * m_rows * count * 4, transcendentals=0),
        name="out_proj",
    )(*o_list, w_out)


def cache_kernel(len_ref, lat_ref, lat_new_ref, pe_ref, pe_new_ref, lat_out_ref, pe_out_ref):
    start = len_ref[pl.program_id(0)]
    for old_ref, new_ref, out_ref, axis in ((lat_ref, lat_new_ref, lat_out_ref, 0), (pe_ref, pe_new_ref, pe_out_ref, 1)):
        new = new_ref[0].astype(F32)
        count = new.shape[axis]
        wide = jnp.concatenate([new, jnp.zeros_like(new)], axis=axis)
        moved = pltpu.roll(wide, start, axis)
        pos = lax.broadcasted_iota(jnp.int32, wide.shape, axis)
        inside = jnp.logical_and(pos >= start, pos < start + count)
        out_ref[0] = jnp.where(inside, moved, old_ref[0].astype(F32)).astype(BF16)


def write_caches(lengths, lat, lat_new, pe_t, pe_new_t):
    spec = lambda arr: pl.BlockSpec((1,) + arr.shape[1:], lambda b, s: (b, 0, 0))
    return pl.pallas_call(
        cache_kernel,
        out_shape=(jax.ShapeDtypeStruct(lat.shape, lat.dtype), jax.ShapeDtypeStruct(pe_t.shape, pe_t.dtype)),
        grid_spec=pltpu.PrefetchScalarGridSpec(
            num_scalar_prefetch=1,
            grid=(lat.shape[0],),
            in_specs=[spec(lat), spec(lat_new), spec(pe_t), spec(pe_new_t)],
            out_specs=(spec(lat), spec(pe_t)),
        ),
        compiler_params=pltpu.CompilerParams(dimension_semantics=("arbitrary",)),
        cost_estimate=pl.CostEstimate(flops=20_000_000, bytes_accessed=2 * lat.size * 2, transcendentals=0),
        name="write_caches",
    )(lengths, lat, lat_new, pe_t, pe_new_t)


def solution(mesh):
    tp = mesh.shape["tp"]
    to_partner = [(i, i ^ 1) for i in range(tp)]
    to_chip = [(i, i ^ 2) for i in range(tp)]

    def partner(value):
        return lax.ppermute(value, "tp", to_partner)

    def other_chip(value):
        return lax.ppermute(value, "tp", to_chip)

    def step(hidden, lengths, rope_cos, rope_sin, cache_lat, cache_pe, norm_in, w_dq, norm_q, w_dkv, norm_kv, w_uq, w_uk, w_uv, w_out):
        me = lax.axis_index("tp")
        n_seq, n_tok, model_dim = hidden.shape
        kv_rank, _, nope = w_uk.shape
        rope_dim = cache_pe.shape[2]
        n_new = rope_cos.shape[1]
        prefix = cache_lat.shape[1] - n_new
        q_rank = w_dq.shape[1]
        scale = (nope + rope_dim) ** -0.5

        normed = rms_norm(hidden.astype(F32), norm_in).astype(BF16).reshape(n_seq * n_tok, model_dim)
        kv_proj = jnp.dot(normed, w_dkv, preferred_element_type=F32).reshape(n_seq, n_tok, kv_rank + rope_dim)
        my_cos = lax.dynamic_slice_in_dim(rope_cos, me * n_tok, n_tok, axis=1)
        my_sin = lax.dynamic_slice_in_dim(rope_sin, me * n_tok, n_tok, axis=1)
        my_lat = rms_norm(kv_proj[..., :kv_rank], norm_kv).astype(BF16)
        my_pe = apply_rope(kv_proj[..., kv_rank:], my_cos, my_sin).astype(BF16)
        my_kv = jnp.concatenate([my_lat, my_pe], axis=-1)
        my_q = rms_norm(jnp.dot(normed, w_dq, preferred_element_type=F32), norm_q).astype(BF16).reshape(n_seq, n_tok, q_rank)

        def gather(value):
            far = other_chip(value)
            near = partner(value)
            return [value, near, far, partner(far)]

        kv_rel = jnp.stack(gather(my_kv))
        kv_true = jnp.concatenate([lax.dynamic_index_in_dim(kv_rel, me ^ j, keepdims=False) for j in range(tp)], axis=1)
        lat_new = kv_true[..., :kv_rank]
        pe_new = kv_true[..., kv_rank:]
        q_rel = [gather(my_q[b]) for b in range(n_seq)]

        row = jnp.arange(prefix)
        alive = row[None, :] < lengths[:, None]
        old_lat = jnp.where(alive[..., None], cache_lat[:, :prefix], 0)
        old_pe = jnp.where(alive[..., None], cache_pe[:, :prefix], 0)
        k_old, v_old = latent_project(old_lat, w_uk, w_uv)
        k_new, v_new = latent_project(lat_new, w_uk, w_uv)
        bias = jnp.where(alive, 0.0, NEG).astype(BF16)[..., None]
        pad_old = jnp.zeros((n_seq, prefix, nope - rope_dim - 1), BF16)
        pad_new = jnp.zeros((n_seq, n_new, nope - rope_dim), BF16)
        r_cat = jnp.concatenate([
            jnp.concatenate([old_pe, bias, pad_old], axis=-1),
            jnp.concatenate([pe_new, pad_new], axis=-1)], axis=1)

        def queries(q_lat):
            return jnp.einsum("qhd,tq->hdt", w_uq, q_lat, preferred_element_type=F32)

        def attend(rel, b, q, q_tile):
            blocks = (me ^ rel, me ^ (rel + 1))
            scal = jnp.stack([blocks[0], blocks[1], blocks[0] // 2]).astype(jnp.int32)
            cut = lambda tab: jnp.concatenate([lax.dynamic_slice_in_dim(tab[b], k * n_tok, n_tok, axis=0) for k in blocks], axis=0).T
            return attention(scal, q, q_tile, b, k_old, k_new, v_old, v_new, r_cat[b], cut(rope_cos), cut(rope_sin), scale)

        def after(value, *deps):
            return lax.optimization_barrier((value,) + deps)[0]

        def tokens(rel):
            return jnp.concatenate([q_rel[b][k] for b in range(n_seq) for k in (rel, rel + 1)], axis=0)

        arrived = []
        pending = []

        def send_one():
            near_part, came = pending.pop(0)
            summed = near_part + came
            arrived.append(other_chip(summed))
            return summed

        q_far = queries(tokens(2))
        o_far = []
        for b in range(n_seq):
            o_far.append(attend(2, b, after(q_far, *o_far), b))
        first = 0
        q_own = None
        for j, width in enumerate(FAR_WIDTHS):
            deps = ()
            if j == 1:
                q_own = queries(after(tokens(0), near_part))
                deps = (near_part, q_own, send_one())
            elif j > 1:
                deps = (near_part, send_one())
            near_part, far_part = out_proj([after(o_far[0], *deps), o_far[1]], w_out, first, width)
            pending.append((near_part, partner(far_part)))
            first += width
        dep = (near_part,)
        o_own = []
        for b in range(n_seq):
            o_own.append(attend(0, b, after(q_own, *dep), b))
            dep = (o_own[-1],) + ((send_one(),) if pending else ())
        flat = hidden.reshape(n_seq * n_tok, model_dim)
        base = []
        first = 0
        for width in OWN_WIDTHS:
            own_part, partner_part = out_proj([after(o_own[0], *dep), o_own[1]], w_out, first, width)
            dep = (own_part,)
            base.append(own_part + partner(partner_part))
            first += width
        total = jnp.concatenate(base, axis=1) + flat.astype(F32) + jnp.concatenate(arrived, axis=1)
        out = total.astype(BF16).reshape(hidden.shape)
        lat_all, pe_all_t = write_caches(lengths, cache_lat, lat_new, cache_pe.transpose(0, 2, 1), pe_new.transpose(0, 2, 1))
        pe_all = pe_all_t.transpose(0, 2, 1)
        return out, lat_all, pe_all

    spec_tok = P("dp", "tp", None)
    spec_len = P("dp")
    spec_seq = P("dp", None, None)
    spec_vec = P(None)
    spec_mat = P(None, None)
    spec_head = P(None, "tp", None)
    spec_rows = P("tp", None)
    in_specs = (spec_tok, spec_len, spec_seq, spec_seq, spec_seq, spec_seq, spec_vec, spec_mat, spec_vec, spec_mat, spec_vec, spec_head, spec_head, spec_head, spec_rows)
    return jax.shard_map(step, mesh=mesh, in_specs=in_specs, out_specs=(spec_tok, spec_seq, spec_seq), check_vma=False)
```

```python
import functools

import jax
import jax.numpy as jnp
from jax import lax
from jax.experimental import pallas as pl
from jax.experimental.pallas import tpu as pltpu
from jax.sharding import PartitionSpec as P


F32 = jnp.float32
BF16 = jnp.bfloat16
NEG = -1e30
LOG2E = 1.4426950408889634
COL_TILE = 512
FAR_WIDTHS = (1536, 2048, 3584)
OWN_WIDTHS = (4096, 3072)
HEADS_PER_STEP = 8
W_SLOTS = 4


def rms_norm(values, gain_vec):
    inv_rms = lax.rsqrt(jnp.mean(values * values, axis=-1, keepdims=True) + 1e-6)
    return values * inv_rms * gain_vec


def apply_rope(values, cos_tab, sin_tab):
    half_dim = values.shape[-1] // 2
    lower_half = values[..., :half_dim]
    upper_half = values[..., half_dim:]
    return jnp.concatenate([lower_half * cos_tab - upper_half * sin_tab, upper_half * cos_tab + lower_half * sin_tab], axis=-1)


def latent_kernel(lat_ref, wk_ref, wv_ref, k_ref, v_ref, wk_buf, wv_buf):
    n_seq, heads, _, dim = k_ref.shape
    wk_buf[...] = jnp.swapaxes(wk_ref[...].astype(F32), 0, 1).astype(BF16)
    wv_buf[...] = jnp.swapaxes(wv_ref[...].astype(F32), 0, 1).astype(BF16)
    for h in range(0, heads, 2):
        wk = jnp.concatenate([wk_buf[h], wk_buf[h + 1]], axis=1)
        wv = jnp.concatenate([wv_buf[h], wv_buf[h + 1]], axis=1)
        for b in range(n_seq):
            lat = lat_ref[b]
            keys = jnp.dot(lat, wk, preferred_element_type=F32)
            values = jnp.dot(lat, wv, preferred_element_type=F32)
            for i in range(2):
                k_ref[b, h + i] = keys[:, i * dim:(i + 1) * dim].astype(BF16)
                v_ref[b, h + i] = values[:, i * dim:(i + 1) * dim].T.astype(BF16)


def latent_project(lat, w_uk, w_uv):
    n_seq, n_rows, rank = lat.shape
    _, n_heads, dim = w_uk.shape
    group = 8
    w_spec = pl.BlockSpec((rank, group, dim), lambda g: (0, g, 0))
    return pl.pallas_call(
        latent_kernel,
        out_shape=(
            jax.ShapeDtypeStruct((n_seq, n_heads, n_rows, dim), BF16),
            jax.ShapeDtypeStruct((n_seq, n_heads, dim, n_rows), BF16),
        ),
        grid=(n_heads // group,),
        in_specs=[pl.BlockSpec(lat.shape, lambda g: (0, 0, 0)), w_spec, w_spec],
        out_specs=(
            pl.BlockSpec((n_seq, group, n_rows, dim), lambda g: (0, g, 0, 0)),
            pl.BlockSpec((n_seq, group, dim, n_rows), lambda g: (0, g, 0, 0)),
        ),
        scratch_shapes=[pltpu.VMEM((group, rank, dim), BF16), pltpu.VMEM((group, rank, dim), BF16)],
        compiler_params=pltpu.CompilerParams(dimension_semantics=("arbitrary",)),
        cost_estimate=pl.CostEstimate(flops=4 * n_seq * n_rows * rank * n_heads * dim, bytes_accessed=25_000_000, transcendentals=0),
        name="latent_project",
    )(lat, w_uk, w_uv)


def attention_kernel(scal_ref, q_ref, k_old_ref, k_new_ref, v_old_ref, v_new_ref, r_ref, cos_ref, sin_ref, o_ref, *, scale):
    heads, _, m_rows = q_ref.shape
    nope = k_old_ref.shape[2]
    prefix = k_old_ref.shape[1]
    rope_half = cos_ref.shape[0]
    blk = m_rows
    factor = scale * LOG2E
    cos_tab = cos_ref[...]
    sin_tab = sin_ref[...]
    pad_row = lax.broadcasted_iota(jnp.int32, (nope - 2 * rope_half, m_rows), 0)
    ones_row = jnp.where(pad_row == 0, 1.0, 0.0).astype(BF16)
    half = m_rows // 2
    qlane = lax.broadcasted_iota(jnp.int32, (blk, m_rows), 1)
    krow = lax.broadcasted_iota(jnp.int32, (blk, m_rows), 0)
    q_blk0 = scal_ref[0]
    q_blk1 = scal_ref[1]
    base = scal_ref[2] * m_rows
    qpos = jnp.where(qlane < half, q_blk0 * half + qlane, q_blk1 * half + qlane - half) - base
    causal = krow <= qpos

    def body(new_blocks):
        for h in range(heads):
            low = q_ref[h, nope:nope + rope_half, :]
            high = q_ref[h, nope + rope_half:, :]
            q_cat = jnp.concatenate([
                q_ref[h, :nope, :].astype(BF16),
                (low * cos_tab - high * sin_tab).astype(BF16),
                (high * cos_tab + low * sin_tab).astype(BF16),
                ones_row], axis=0)
            scores = []
            for i in range(prefix // blk + new_blocks):
                start = i * blk
                if start < prefix:
                    k_part = k_old_ref[h, start:start + blk, :]
                else:
                    k_part = k_new_ref[h, start - prefix:start - prefix + blk, :]
                k_cat = jnp.concatenate([k_part, r_ref[start:start + blk, :]], axis=1)
                s = jnp.dot(k_cat, q_cat, preferred_element_type=F32)
                if i == prefix // blk + new_blocks - 1:
                    s = jnp.where(causal, s, NEG)
                scores.append(s)
            top = functools.reduce(jnp.maximum, scores)
            top = jnp.max(top, axis=0, keepdims=True)
            total = None
            out = None
            for i, s in enumerate(scores):
                start = i * blk
                e = jnp.exp2((s - top) * factor)
                part = jnp.sum(e, axis=0, keepdims=True)
                total = part if total is None else total + part
                if start < prefix:
                    v_part = v_old_ref[h, :, start:start + blk]
                else:
                    v_part = v_new_ref[h, :, start - prefix:start - prefix + blk]
                o_part = jnp.dot(v_part, e.astype(BF16), preferred_element_type=F32)
                out = o_part if out is None else out + o_part
            out = out * (1.0 / total)
            o_ref[:, h * nope:(h + 1) * nope] = out.T.astype(BF16)

    for c in range(v_new_ref.shape[2] // blk):
        @pl.when(scal_ref[2] == c)
        def _(c=c):
            body(c + 1)


def attention(scal, q, q_tile, seq, k_old, k_new, v_old, v_new, r_cat, cos_tab, sin_tab, scale):
    n_heads, q_dim, _ = q.shape
    m_rows = cos_tab.shape[1]
    prefix, nope = k_old.shape[2:]
    n_new = k_new.shape[2]
    hb = HEADS_PER_STEP
    flops = 2 * n_heads * m_rows * (prefix + n_new) * (256 + 128)
    head_blk = lambda *shape: pl.BlockSpec((None, hb) + shape, lambda g, s: (seq, g, 0, 0))
    whole = lambda *shape: pl.BlockSpec(shape, lambda g, s: (0, 0))
    return pl.pallas_call(
        functools.partial(attention_kernel, scale=scale),
        out_shape=jax.ShapeDtypeStruct((m_rows, n_heads * nope), BF16),
        grid_spec=pltpu.PrefetchScalarGridSpec(
            num_scalar_prefetch=1,
            grid=(n_heads // hb,),
            in_specs=[
                pl.BlockSpec((hb, q_dim, m_rows), lambda g, s: (g, 0, q_tile)),
                head_blk(prefix, nope),
                head_blk(n_new, nope),
                head_blk(nope, prefix),
                head_blk(nope, n_new),
                whole(*r_cat.shape),
                whole(*cos_tab.shape),
                whole(*sin_tab.shape),
            ],
            out_specs=pl.BlockSpec((m_rows, hb * nope), lambda g, s: (0, g)),
        ),
        compiler_params=pltpu.CompilerParams(dimension_semantics=("arbitrary",)),
        cost_estimate=pl.CostEstimate(flops=flops, bytes_accessed=30_000_000, transcendentals=n_heads * m_rows * (prefix + n_new)),
        name="attention",
    )(scal, q, k_old, k_new, v_old, v_new, r_cat, cos_tab, sin_tab)


def out_proj_kernel(*refs, n_in, first):
    o_hbm = refs[:n_in]
    w_hbm, near_ref, far_ref, o_buf, w_buf, o_sems, w_sems = refs[n_in:]
    j = pl.program_id(0)
    tiles = pl.num_programs(0)
    slots = w_buf.shape[0]
    m_rows = o_buf.shape[0] // n_in
    half = m_rows // 2

    def weights(tile, slot):
        col = pl.multiple_of((tile + first) * COL_TILE, COL_TILE)
        return pltpu.make_async_copy(w_hbm.at[:, pl.ds(col, COL_TILE)], w_buf.at[slot], w_sems.at[slot])

    @pl.when(j == 0)
    def _():
        weights(0, 0).start()
        loads = [pltpu.make_async_copy(o_hbm[i], o_buf.at[pl.ds(i * m_rows, m_rows)], o_sems.at[i]) for i in range(n_in)]
        for load in loads:
            load.start()
        for slot in range(1, slots):
            weights(slot, slot).start()
        for load in loads:
            load.wait()

    slot = lax.rem(j, slots)
    weights(j, slot).wait()
    prod = jnp.dot(o_buf[:, :], w_buf[slot], preferred_element_type=F32)
    for i in range(n_in):
        near_ref[i * half:(i + 1) * half, :] = prod[2 * i * half:(2 * i + 1) * half]
        far_ref[i * half:(i + 1) * half, :] = prod[(2 * i + 1) * half:(2 * i + 2) * half]

    @pl.when(j + slots < tiles)
    def _():
        weights(j + slots, slot).start()


def out_proj(o_list, w_out, first, count):
    m_rows, depth = o_list[0].shape
    n_in = len(o_list)
    half = m_rows // 2
    tiles = count // COL_TILE
    slots = min(W_SLOTS, tiles)
    out = jax.ShapeDtypeStruct((n_in * half, count), F32)
    raw = pl.BlockSpec(memory_space=pl.ANY)
    out_spec = pl.BlockSpec((n_in * half, COL_TILE), lambda j: (0, j))
    return pl.pallas_call(
        functools.partial(out_proj_kernel, n_in=n_in, first=first // COL_TILE),
        out_shape=(out, out),
        grid=(tiles,),
        in_specs=[raw] * (n_in + 1),
        out_specs=(out_spec, out_spec),
        scratch_shapes=[
            pltpu.VMEM((n_in * m_rows, depth), BF16),
            pltpu.VMEM((slots, depth, COL_TILE), BF16),
            pltpu.SemaphoreType.DMA((n_in,)),
            pltpu.SemaphoreType.DMA((slots,)),
        ],
        compiler_params=pltpu.CompilerParams(dimension_semantics=("arbitrary",)),
        cost_estimate=pl.CostEstimate(flops=2 * n_in * m_rows * depth * count, bytes_accessed=depth * count * 2 + n_in * m_rows * count * 4, transcendentals=0),
        name="out_proj",
    )(*o_list, w_out)


def cache_kernel(len_ref, lat_ref, lat_new_ref, pe_ref, pe_new_ref, lat_out_ref, pe_out_ref):
    start = len_ref[pl.program_id(0)]
    for old_ref, new_ref, out_ref, axis in ((lat_ref, lat_new_ref, lat_out_ref, 0), (pe_ref, pe_new_ref, pe_out_ref, 1)):
        new = new_ref[0].astype(F32)
        count = new.shape[axis]
        wide = jnp.concatenate([new, jnp.zeros_like(new)], axis=axis)
        moved = pltpu.roll(wide, start, axis)
        pos = lax.broadcasted_iota(jnp.int32, wide.shape, axis)
        inside = jnp.logical_and(pos >= start, pos < start + count)
        out_ref[0] = jnp.where(inside, moved, old_ref[0].astype(F32)).astype(BF16)


def write_caches(lengths, lat, lat_new, pe_t, pe_new_t):
    spec = lambda arr: pl.BlockSpec((1,) + arr.shape[1:], lambda b, s: (b, 0, 0))
    return pl.pallas_call(
        cache_kernel,
        out_shape=(jax.ShapeDtypeStruct(lat.shape, lat.dtype), jax.ShapeDtypeStruct(pe_t.shape, pe_t.dtype)),
        grid_spec=pltpu.PrefetchScalarGridSpec(
            num_scalar_prefetch=1,
            grid=(lat.shape[0],),
            in_specs=[spec(lat), spec(lat_new), spec(pe_t), spec(pe_new_t)],
            out_specs=(spec(lat), spec(pe_t)),
        ),
        compiler_params=pltpu.CompilerParams(dimension_semantics=("arbitrary",)),
        cost_estimate=pl.CostEstimate(flops=20_000_000, bytes_accessed=2 * lat.size * 2, transcendentals=0),
        name="write_caches",
    )(lengths, lat, lat_new, pe_t, pe_new_t)


def solution(mesh):
    tp = mesh.shape["tp"]
    to_partner = [(i, i ^ 1) for i in range(tp)]
    to_chip = [(i, i ^ 2) for i in range(tp)]

    def partner(value):
        return lax.ppermute(value, "tp", to_partner)

    def other_chip(value):
        return lax.ppermute(value, "tp", to_chip)

    def step(hidden, lengths, rope_cos, rope_sin, cache_lat, cache_pe, norm_in, w_dq, norm_q, w_dkv, norm_kv, w_uq, w_uk, w_uv, w_out):
        me = lax.axis_index("tp")
        n_seq, n_tok, model_dim = hidden.shape
        kv_rank, _, nope = w_uk.shape
        rope_dim = cache_pe.shape[2]
        n_new = rope_cos.shape[1]
        prefix = cache_lat.shape[1] - n_new
        q_rank = w_dq.shape[1]
        scale = (nope + rope_dim) ** -0.5

        normed = rms_norm(hidden.astype(F32), norm_in).astype(BF16).reshape(n_seq * n_tok, model_dim)
        kv_proj = jnp.dot(normed, w_dkv, preferred_element_type=F32).reshape(n_seq, n_tok, kv_rank + rope_dim)
        my_cos = lax.dynamic_slice_in_dim(rope_cos, me * n_tok, n_tok, axis=1)
        my_sin = lax.dynamic_slice_in_dim(rope_sin, me * n_tok, n_tok, axis=1)
        my_lat = rms_norm(kv_proj[..., :kv_rank], norm_kv).astype(BF16)
        my_pe = apply_rope(kv_proj[..., kv_rank:], my_cos, my_sin).astype(BF16)
        my_kv = jnp.concatenate([my_lat, my_pe], axis=-1)
        my_q = rms_norm(jnp.dot(normed, w_dq, preferred_element_type=F32), norm_q).astype(BF16).reshape(n_seq, n_tok, q_rank)

        def gather(value):
            far = other_chip(value)
            near = partner(value)
            return [value, near, far, partner(far)]

        kv_rel = jnp.stack(gather(my_kv))
        kv_true = jnp.concatenate([lax.dynamic_index_in_dim(kv_rel, me ^ j, keepdims=False) for j in range(tp)], axis=1)
        lat_new = kv_true[..., :kv_rank]
        pe_new = kv_true[..., kv_rank:]
        q_rel = [gather(my_q[b]) for b in range(n_seq)]

        row = jnp.arange(prefix)
        alive = row[None, :] < lengths[:, None]
        old_lat = jnp.where(alive[..., None], cache_lat[:, :prefix], 0)
        old_pe = jnp.where(alive[..., None], cache_pe[:, :prefix], 0)
        k_old, v_old = latent_project(old_lat, w_uk, w_uv)
        k_new, v_new = latent_project(lat_new, w_uk, w_uv)
        bias = jnp.where(alive, 0.0, NEG).astype(BF16)[..., None]
        pad_old = jnp.zeros((n_seq, prefix, nope - rope_dim - 1), BF16)
        pad_new = jnp.zeros((n_seq, n_new, nope - rope_dim), BF16)
        r_cat = jnp.concatenate([
            jnp.concatenate([old_pe, bias, pad_old], axis=-1),
            jnp.concatenate([pe_new, pad_new], axis=-1)], axis=1)

        def queries(q_lat):
            return jnp.einsum("qhd,tq->hdt", w_uq, q_lat, preferred_element_type=F32)

        def attend(rel, b, q, q_tile):
            blocks = (me ^ rel, me ^ (rel + 1))
            scal = jnp.stack([blocks[0], blocks[1], blocks[0] // 2]).astype(jnp.int32)
            cut = lambda tab: jnp.concatenate([lax.dynamic_slice_in_dim(tab[b], k * n_tok, n_tok, axis=0) for k in blocks], axis=0).T
            return attention(scal, q, q_tile, b, k_old, k_new, v_old, v_new, r_cat[b], cut(rope_cos), cut(rope_sin), scale)

        def after(value, *deps):
            return lax.optimization_barrier((value,) + deps)[0]

        def tokens(rel):
            return jnp.concatenate([q_rel[b][k] for b in range(n_seq) for k in (rel, rel + 1)], axis=0)

        arrived = []
        pending = []

        def send_one():
            near_part, came = pending.pop(0)
            summed = near_part + came
            arrived.append(other_chip(summed))
            return summed

        q_far = queries(tokens(2))
        o_far = []
        for b in range(n_seq):
            o_far.append(attend(2, b, after(q_far, *o_far), b))
        first = 0
        q_own = None
        for j, width in enumerate(FAR_WIDTHS):
            deps = ()
            if j == 1:
                q_own = queries(after(tokens(0), near_part))
                deps = (near_part, q_own, send_one())
            elif j > 1:
                deps = (near_part, send_one())
            near_part, far_part = out_proj([after(o_far[0], *deps), o_far[1]], w_out, first, width)
            pending.append((near_part, partner(far_part)))
            first += width
        dep = (near_part,)
        o_own = []
        for b in range(n_seq):
            o_own.append(attend(0, b, after(q_own, *dep), b))
            dep = (o_own[-1],) + ((send_one(),) if pending else ())
        flat = hidden.reshape(n_seq * n_tok, model_dim)
        base = []
        first = 0
        for width in OWN_WIDTHS:
            own_part, partner_part = out_proj([after(o_own[0], *dep), o_own[1]], w_out, first, width)
            dep = (own_part,)
            base.append(own_part + partner(partner_part))
            first += width
        total = jnp.concatenate(base, axis=1) + flat.astype(F32) + jnp.concatenate(arrived, axis=1)
        out = total.astype(BF16).reshape(hidden.shape)
        lat_all, pe_all_t = write_caches(lengths, cache_lat, lat_new, cache_pe.transpose(0, 2, 1), pe_new.transpose(0, 2, 1))
        pe_all = pe_all_t.transpose(0, 2, 1)
        return out, lat_all, pe_all

    spec_tok = P("dp", "tp", None)
    spec_len = P("dp")
    spec_seq = P("dp", None, None)
    spec_vec = P(None)
    spec_mat = P(None, None)
    spec_head = P(None, "tp", None)
    spec_rows = P("tp", None)
    in_specs = (spec_tok, spec_len, spec_seq, spec_seq, spec_seq, spec_seq, spec_vec, spec_mat, spec_vec, spec_mat, spec_vec, spec_head, spec_head, spec_head, spec_rows)
    return jax.shard_map(step, mesh=mesh, in_specs=in_specs, out_specs=(spec_tok, spec_seq, spec_seq), check_vma=False)
```
